16 devices in a mesh: vp: 2 (over z), dp: 8 (over y, x, core).
Axes of the slice: x: 2, y: 2, z: 2, core: 2. Of those that a mesh axis runs over, the one named last changes fastest.
Arguments:
- hidden: bfloat16 [64, 512, 768], P('dp')
- mask_pos: int32 [64, 77], P('dp')
- labels: int32 [64, 77], P('dp')
- w_trans: bfloat16 [768, 768], replicated
- b_trans: float32 [768], replicated
- ln_gain: float32 [768], replicated
- ln_bias: float32 [768], replicated
- emb_table: bfloat16 [50304, 768], P('vp')
- b_vocab: float32 [50304], P('vp')
Outputs:
- output 1: float32 [], replicated
- output 2: bfloat16 [64, 512, 768], P('dp')
- output 3: float32 [768, 768], replicated
- output 4: float32 [768], replicated
- output 5: float32 [768], replicated
- output 6: float32 [768], replicated
- output 7: float32 [50304, 768], P('vp')
- output 8: float32 [50304], P('vp')
All inputs are finite; a program needn't handle non-finite values.
Results may differ from the reference program's by a relative error of at most 0.0106917.
Values sent between devices are 32-bit elements.
A program may use at most 1 GiB of HBM per device.

```python
import jax
import jax.numpy as jnp
from jax import lax

HIDDEN = 768
VOCAB_PAD = 50304
VOCAB_REAL = 50265
SEQ_LEN = 512
N_MASKS = 77
BATCH_ALL = 64
SHARDS = 2
LOG_VOCAB = (VOCAB_REAL - 1).bit_length()
LN_EPS = 1e-5
PAD_BIAS = -1.0e9


def head_norm(pre_act, ln_gain, ln_bias):
    gelu_out = jax.nn.gelu(pre_act, approximate=False)
    row_mean = jnp.mean(gelu_out, axis=-1, keepdims=True)
    centered = gelu_out - row_mean
    row_var = jnp.mean(centered * centered, axis=-1, keepdims=True)
    return centered * lax.rsqrt(row_var + LN_EPS) * ln_gain + ln_bias


def setup_inputs(seed: int = 0) -> dict:
    sub_keys = jax.random.split(jax.random.key(seed), 12)
    hidden = jax.random.normal(sub_keys[0], (BATCH_ALL, SEQ_LEN, HIDDEN), jnp.float32).astype(jnp.bfloat16)

    def draw_row(row_key):
        return jax.random.permutation(row_key, SEQ_LEN)[:N_MASKS]

    mask_pos = jax.vmap(draw_row)(jax.random.split(sub_keys[1], BATCH_ALL)).astype(jnp.int32)
    label_exp = jax.random.randint(sub_keys[2], (BATCH_ALL, N_MASKS), 0, LOG_VOCAB + 1)
    label_top = jnp.minimum(jnp.left_shift(jnp.ones_like(label_exp), label_exp), VOCAB_REAL)
    labels = jax.random.randint(sub_keys[3], (BATCH_ALL, N_MASKS), 0, label_top)
    labels = labels.at[0, 0].set(VOCAB_REAL - 1).astype(jnp.int32)
    w_trans = (jax.random.normal(sub_keys[4], (HIDDEN, HIDDEN), jnp.float32) * HIDDEN ** -0.5).astype(jnp.bfloat16)
    b_trans = 0.5 * jax.random.normal(sub_keys[5], (HIDDEN,), jnp.float32)
    ln_gain = 1.0 + 0.3 * jax.random.normal(sub_keys[6], (HIDDEN,), jnp.float32)
    ln_bias = 0.3 * jax.random.normal(sub_keys[7], (HIDDEN,), jnp.float32)
    emb_table = (jax.random.normal(sub_keys[8], (VOCAB_PAD, HIDDEN), jnp.float32) * HIDDEN ** -0.5).astype(jnp.bfloat16)
    bias_slope = jax.random.uniform(sub_keys[9], (), jnp.float32, 0.3, 0.6)
    bias_noise = jax.random.normal(sub_keys[10], (VOCAB_PAD,), jnp.float32)
    vocab_ids = jnp.arange(VOCAB_PAD)
    b_vocab = 0.5 * bias_noise - bias_slope * jnp.log1p(vocab_ids.astype(jnp.float32))
    b_vocab = jnp.where(vocab_ids < VOCAB_REAL, b_vocab, PAD_BIAS).astype(jnp.float32)
    return {"hidden": hidden, "mask_pos": mask_pos, "labels": labels, "w_trans": w_trans, "b_trans": b_trans, "ln_gain": ln_gain, "ln_bias": ln_bias, "emb_table": emb_table, "b_vocab": b_vocab}


def reference(hidden, mask_pos, labels, w_trans, b_trans, ln_gain, ln_bias, emb_table, b_vocab):
    n_rows = hidden.shape[0]
    n_tokens = n_rows * N_MASKS
    shard_rows = VOCAB_PAD // SHARDS
    masked_h = jnp.take_along_axis(hidden, mask_pos[:, :, None], axis=1).reshape(n_tokens, HIDDEN)
    pre_act = jnp.dot(masked_h, w_trans, preferred_element_type=jnp.float32) + b_trans
    u_norm, head_vjp = jax.vjp(head_norm, pre_act, ln_gain, ln_bias)
    u_bf16 = u_norm.astype(jnp.bfloat16)
    flat_labels = labels.reshape(n_tokens)
    emb_blocks = emb_table.reshape(SHARDS, shard_rows, HIDDEN)
    bias_blocks = b_vocab.reshape(SHARDS, shard_rows)
    row_starts = jnp.arange(SHARDS) * shard_rows
    row_ids = jnp.arange(shard_rows)

    def block_logits(emb_block, bias_block):
        return jnp.dot(u_bf16, emb_block.T, preferred_element_type=jnp.float32) + bias_block

    def block_stats(block):
        emb_block, bias_block, row_start = block
        logits = block_logits(emb_block, bias_block)
        local_max = jnp.max(logits, axis=1)
        local_sum = jnp.sum(jnp.exp(logits - local_max[:, None]), axis=1)
        is_label = (flat_labels - row_start)[:, None] == row_ids[None, :]
        label_logit = jnp.sum(jnp.where(is_label, logits, 0.0), axis=1)
        return local_max, local_sum, label_logit

    block_max, block_sum, block_label = lax.map(block_stats, (emb_blocks, bias_blocks, row_starts))
    global_max = jnp.max(block_max, axis=0)
    log_norm = global_max + jnp.log(jnp.sum(block_sum * jnp.exp(block_max - global_max), axis=0))
    mlm_loss = jnp.mean(log_norm - jnp.sum(block_label, axis=0))

    def block_grads(block):
        emb_block, bias_block, row_start = block
        logits = block_logits(emb_block, bias_block)
        is_label = (flat_labels - row_start)[:, None] == row_ids[None, :]
        d_logits = (jnp.exp(logits - log_norm[:, None]) - is_label.astype(jnp.float32)) / n_tokens
        d_logits_bf = d_logits.astype(jnp.bfloat16)
        d_emb_block = jnp.dot(d_logits_bf.T, u_bf16, preferred_element_type=jnp.float32)
        du_part = jnp.dot(d_logits_bf, emb_block, preferred_element_type=jnp.float32).astype(jnp.bfloat16)
        return d_emb_block, jnp.sum(d_logits, axis=0), du_part

    d_emb_blocks, d_bias_blocks, du_parts = lax.map(block_grads, (emb_blocks, bias_blocks, row_starts))
    d_unorm = jnp.sum(du_parts.astype(jnp.float32), axis=0)
    d_pre, d_ln_gain, d_ln_bias = head_vjp(d_unorm)
    d_pre_bf = d_pre.astype(jnp.bfloat16)
    d_w_trans = jnp.dot(masked_h.T, d_pre_bf, preferred_element_type=jnp.float32)
    d_b_trans = jnp.sum(d_pre, axis=0)
    d_masked = jnp.dot(d_pre_bf, w_trans.T, preferred_element_type=jnp.float32).astype(jnp.bfloat16)
    row_index = jnp.arange(n_rows)[:, None]
    d_hidden = jnp.zeros_like(hidden).at[row_index, mask_pos].set(d_masked.reshape(n_rows, N_MASKS, HIDDEN))
    return (mlm_loss, d_hidden, d_w_trans, d_b_trans, d_ln_gain, d_ln_bias, d_emb_blocks.reshape(VOCAB_PAD, HIDDEN), d_bias_blocks.reshape(VOCAB_PAD))
```

```python
import functools

import jax
import jax.numpy as jnp
from jax import lax
from jax.experimental import pallas as pl
from jax.experimental.pallas import tpu as pltpu
from jax.sharding import PartitionSpec as P


LN_EPS = 1e-5

BF16, F32, I32 = jnp.bfloat16, jnp.float32, jnp.int32
SLOTS = 80
VT = 2304
CHUNK, ROWS = 768, 128
SHARE_CHUNKS, SHARE_TILE = 4, 528
LOCAL_TILES, LOCAL_TILE = 6, 688
LOCAL_CALLS = 3
TOK_CHUNK = 1280
VMEM_ROWS = 44
COST_SCALE = 4
OFF = 1e30
MIB = 2 ** 20


def head_norm(pre_act, ln_gain, ln_bias):
    gelu_out = jax.nn.gelu(pre_act, approximate=False)
    row_mean = jnp.mean(gelu_out, axis=-1, keepdims=True)
    centered = gelu_out - row_mean
    row_var = jnp.mean(centered * centered, axis=-1, keepdims=True)
    return centered * lax.rsqrt(row_var + LN_EPS) * ln_gain + ln_bias


def dot_nt(a, b):
    return lax.dot_general(a, b, (((1,), (1,)), ((), ())), preferred_element_type=F32)


def to_lanes(row):
    return jnp.broadcast_to(row, (128, row.shape[1])).T


def stats_kernel(n_steps, u_ref, emb_ref, bias_ref, col_ref, lab_row_ref, logit_ref, stat_ref, m_ref, s_ref, t_ref, lab_ref):
    step = pl.program_id(0)
    n_own = u_ref.shape[0]

    @pl.when(step == 0)
    def _():
        m_ref[...] = jnp.full_like(m_ref, -1e38)
        s_ref[...] = jnp.zeros_like(s_ref)
        t_ref[...] = jnp.zeros_like(t_ref)
        lab_ref[...] = to_lanes(lab_row_ref[...])

    for q in range(VT // CHUNK):
        cs = slice(q * CHUNK, (q + 1) * CHUNK)
        block = dot_nt(u_ref[...], emb_ref[cs, :]) + bias_ref[0, :, cs]
        logit_ref[0, :, cs] = block
        for r in range(n_own // ROWS):
            rs = slice(r * ROWS, (r + 1) * ROWS)
            cols = [block[rs, k * 128:(k + 1) * 128] for k in range(CHUNK // 128)]
            m_old = m_ref[rs, :]
            m_new = functools.reduce(jnp.maximum, cols, m_old)
            total = s_ref[rs, :] * jnp.exp(m_old - m_new)
            label = t_ref[rs, :]
            lab = lab_ref[rs, :]
            for k, col in enumerate(cols):
                total += jnp.exp(col - m_new)
                ids = col_ref[0, :, q * CHUNK + k * 128:q * CHUNK + (k + 1) * 128]
                label += jnp.where(ids == lab, col, 0.0)
            m_ref[rs, :] = m_new
            s_ref[rs, :] = total
            t_ref[rs, :] = label

    @pl.when(step == n_steps - 1)
    def _():
        m_new = m_ref[...]
        top = jnp.max(m_new, axis=1, keepdims=True)
        mass = jnp.sum(s_ref[...] * jnp.exp(m_new - top), axis=1, keepdims=True)
        target = jnp.sum(t_ref[...], axis=1, keepdims=True)
        lane = lax.broadcasted_iota(I32, m_new.shape, 1)
        stat_ref[...] = jnp.where(lane == 0, top, jnp.where(lane == 1, mass, target)).T[:8]


def du_kernel(n_steps, inv_n, logit_ref, emb_ref, col_ref, norm_row_ref, lab_row_ref, du_ref, db_ref, acc_ref, gb_ref, norm_ref, lab_ref):
    step = pl.program_id(0)
    n_own = acc_ref.shape[0]

    @pl.when(step == 0)
    def _():
        acc_ref[...] = jnp.zeros_like(acc_ref)
        norm_ref[...] = to_lanes(norm_row_ref[...])
        lab_ref[...] = to_lanes(lab_row_ref[...])

    wide = lambda x: jnp.concatenate([x] * (CHUNK // 128), axis=1)
    for q in range(VT // CHUNK):
        cs = slice(q * CHUNK, (q + 1) * CHUNK)
        db = jnp.zeros((1, CHUNK), F32)
        for r in range(n_own // ROWS):
            rs = slice(r * ROWS, (r + 1) * ROWS)
            prob = jnp.exp(logit_ref[0, rs, cs] - wide(norm_ref[rs, :]))
            hot = jnp.where(col_ref[0, :, cs] == wide(lab_ref[rs, :]), 1.0, 0.0)
            grad = (prob - hot) * inv_n
            db += jnp.sum(grad, axis=0, keepdims=True)
            gb_ref[rs, cs] = grad.astype(BF16)
        db_ref[0, :, cs] = db
        acc_ref[...] += jnp.dot(gb_ref[:, cs], emb_ref[cs, :], preferred_element_type=F32)

    @pl.when(step == n_steps - 1)
    def _():
        du_ref[...] = acc_ref[...].astype(BF16).astype(F32)


def place_kernel(n_pieces, n_tok, start_ref, *refs):
    pieces, toks, refs = refs[:n_pieces], refs[n_pieces:n_pieces + n_tok], refs[n_pieces + n_tok:]
    bufs, sems = refs[-n_pieces - 1:-1], refs[-1]
    outs = refs[:-n_pieces - 1]
    out_ref = outs[-3] if n_tok else outs[-1]
    copies = []
    for k in range(n_pieces):
        bufs[k][...] = pieces[k][...].astype(BF16)
        rows = pl.ds(pl.multiple_of(start_ref[k] * 16, 16), pieces[k].shape[0])
        copies.append(pltpu.make_async_copy(bufs[k], out_ref.at[rows, :], sems.at[k]))
        copies[-1].start()
    for k in range(n_tok):
        row = pl.ds(start_ref[n_pieces + k], 1)
        outs[-2][row, :] = toks[k][0:1, :]
        outs[-1][row, :] = toks[k][1:2, :]
    for copy in copies:
        copy.wait()


def place(pieces, starts, n_all, table=None, toks=()):
    n = len(pieces)
    width = pieces[0].shape[1]
    extra = [] if table is None else [table]
    shapes = [jax.ShapeDtypeStruct((n_all, width), BF16)]
    specs = [pl.BlockSpec(memory_space=pl.ANY)]
    if toks:
        shapes += [jax.ShapeDtypeStruct((len(toks), toks[0].shape[1]), F32)] * 2
        specs += [pl.BlockSpec(shapes[-1].shape, lambda i, s: (0, 0))] * 2
    whole = lambda p: pl.BlockSpec(p.shape, lambda i, s: (0, 0))
    return pl.pallas_call(
        functools.partial(place_kernel, n, len(toks)),
        grid_spec=pltpu.PrefetchScalarGridSpec(
            num_scalar_prefetch=1,
            grid=(1,),
            in_specs=[whole(p) for p in pieces] + [whole(t) for t in toks] + [pl.BlockSpec(memory_space=pl.ANY)] * len(extra),
            out_specs=specs,
            scratch_shapes=[pltpu.VMEM(p.shape, BF16) for p in pieces] + [pltpu.SemaphoreType.DMA((n,))],
        ),
        out_shape=shapes,
        input_output_aliases={n + len(toks) + 1: 0} if extra else {},
        compiler_params=pltpu.CompilerParams(vmem_limit_bytes=40 * MIB),
        cost_estimate=pl.CostEstimate(flops=5 * 10 ** 9, bytes_accessed=6 * sum(p.size for p in pieces), transcendentals=0),
    )(starts, *pieces, *toks, *extra)


def rows_kernel(cfg, start_ref, emb_ref, bias_ref, u_ref, norm_ref, lab_ref, *refs):
    n_steps, tile, inv_n, n_send, n_copy, aliased = cfg
    arrived, refs = refs[:n_copy], refs[n_copy + (1 if aliased else 0):]
    out_ref, sends, refs = refs[0], refs[1:1 + n_send], refs[1 + n_send:]
    acc_ref, out_sem, send_sem = refs[:3]
    stage, load_sem, store_sem = (refs[3:3 + n_copy], refs[3 + n_copy], refs[4 + n_copy]) if n_copy else ((), None, None)
    step = pl.program_id(0)
    slot = lax.rem(step, 2)
    n_tok = u_ref.shape[0]

    def load(k):
        return pltpu.make_async_copy(arrived[k], stage[k], load_sem.at[k])

    def store(k):
        rows = pl.ds(pl.multiple_of(start_ref[2 * n_steps + k] * 16, 16), arrived[k].shape[0])
        return pltpu.make_async_copy(stage[k], out_ref.at[rows, :], store_sem.at[k])

    @pl.when(step == 0)
    def _():
        for k in range(n_copy):
            load(k).start()

    @pl.when(step == 1)
    def _():
        for k in range(n_copy):
            load(k).wait()
            store(k).start()

    def out_copy(t, which):
        rows = pl.ds(pl.multiple_of(start_ref[t] * 16, 16), tile)
        return pltpu.make_async_copy(acc_ref.at[which], out_ref.at[rows, :], out_sem.at[which])

    def send_copy(t, which):
        rows = pl.ds(pl.multiple_of(t * tile, 16), tile) if n_send == 1 else pl.ds(0, tile)
        target = sends[0] if n_send == 1 else sends[t]
        return pltpu.make_async_copy(acc_ref.at[which], target.at[rows, :], send_sem.at[which])

    @pl.when(step >= 2)
    def _():
        out_copy(step - 2, slot).wait()
        pltpu.make_async_copy(acc_ref.at[slot], sends[0].at[pl.ds(0, tile), :], send_sem.at[slot]).wait()

    row_id = lax.broadcasted_iota(I32, (tile, 1), 0).astype(F32) + (start_ref[step] * 16).astype(F32)
    bias = jnp.concatenate([to_lanes(bias_ref[0])[:tile]] * (TOK_CHUNK // 128), axis=1)
    per = TOK_CHUNK // norm_ref.shape[1]
    for j in range(n_tok // TOK_CHUNK):
        s = slice(j * TOK_CHUNK, (j + 1) * TOK_CHUNK)
        norm = jnp.concatenate([norm_ref[i:i + 1, :] for i in range(j * per, (j + 1) * per)], axis=1)
        lab = jnp.concatenate([lab_ref[i:i + 1, :] for i in range(j * per, (j + 1) * per)], axis=1)
        logit = dot_nt(emb_ref[...], u_ref[s, :]) + bias
        prob = jnp.exp(logit - norm)
        grad = (prob - jnp.where(lab == row_id, 1.0, 0.0)) * inv_n
        part = jnp.dot(grad.astype(BF16), u_ref[s, :], preferred_element_type=F32)
        if j == 0:
            acc_ref[slot] = part
        else:
            acc_ref[slot] += part

    out_copy(step, slot).start()
    if n_send == 1:
        send_copy(step, slot).start()
    else:
        for t in range(n_send):
            @pl.when(step == t)
            def _():
                send_copy(t, t % 2).start()

    @pl.when(step == n_steps - 1)
    def _():
        for k in range(n_copy):
            store(k).wait()
        for t in range(max(0, n_steps - 2), n_steps):
            out_copy(t, t % 2).wait()
            pltpu.make_async_copy(acc_ref.at[t % 2], sends[0].at[pl.ds(0, tile), :], send_sem.at[t % 2]).wait()


def emb_rows(out, starts, blocks, emb, bias, u_all, norm, lab, inv_n, tile, n_steps, n_send, arrived, copy_starts):
    n_tok, width = u_all.shape
    n_rows = emb.shape[0]
    n_copy = len(arrived)
    aliased = out is not None
    cfg = (n_steps, tile, inv_n, n_send, n_copy, aliased)
    table = jnp.concatenate([starts, blocks] + list(copy_starts)).astype(I32)
    any_space = pl.BlockSpec(memory_space=pl.ANY)
    whole = lambda a: pl.BlockSpec(a.shape, lambda i, s: (0, 0))
    send_rows = n_steps * tile if n_send == 1 else tile
    scratch = [pltpu.VMEM((2, tile, width), F32), pltpu.SemaphoreType.DMA((2,)), pltpu.SemaphoreType.DMA((2,))]
    if n_copy:
        scratch += [pltpu.VMEM(a.shape, F32) for a in arrived] + [pltpu.SemaphoreType.DMA((n_copy,))] * 2
    return pl.pallas_call(
        functools.partial(rows_kernel, cfg),
        grid_spec=pltpu.PrefetchScalarGridSpec(
            num_scalar_prefetch=1,
            grid=(n_steps,),
            in_specs=[
                pl.BlockSpec((pl.Element(tile), pl.Element(width)), lambda i, s: (pl.multiple_of(s[i] * 16, 16), 0)),
                pl.BlockSpec((1, 1, bias.shape[2]), lambda i, s: (s[n_steps + i], 0, 0)),
                pl.BlockSpec(memory_space=pltpu.VMEM), whole(norm), whole(lab),
            ] + [any_space] * (n_copy + aliased),
            out_specs=[any_space] * (1 + n_send),
            scratch_shapes=scratch,
        ),
        out_shape=[jax.ShapeDtypeStruct((n_rows, width), F32)] + [jax.ShapeDtypeStruct((send_rows, width), F32)] * n_send,
        input_output_aliases={6 + n_copy: 0} if aliased else {},
        compiler_params=pltpu.CompilerParams(vmem_limit_bytes=VMEM_ROWS * MIB),
        cost_estimate=pl.CostEstimate(
            flops=n_steps * tile * n_tok * width // COST_SCALE, bytes_accessed=n_steps * tile * width * 10, transcendentals=n_steps * tile * n_tok
        ),
    )(table, emb, bias, u_all, norm, lab, *arrived, *([out] if aliased else []))


def copy_kernel(n, start_ref, *refs):
    arrived, out_ref, stage, load_sem, store_sem = refs[:n], refs[n + 1], refs[n + 2:-2], refs[-2], refs[-1]
    loads = [pltpu.make_async_copy(arrived[k], stage[k], load_sem.at[k]) for k in range(n)]
    for load in loads:
        load.start()
    stores = []
    for k in range(n):
        loads[k].wait()
        rows = pl.ds(pl.multiple_of(start_ref[k] * 16, 16), arrived[k].shape[0])
        stores.append(pltpu.make_async_copy(stage[k], out_ref.at[rows, :], store_sem.at[k]))
        stores[-1].start()
    for store in stores:
        store.wait()


def copy_rows(out, arrived, starts):
    n = len(arrived)
    return pl.pallas_call(
        functools.partial(copy_kernel, n),
        grid_spec=pltpu.PrefetchScalarGridSpec(
            num_scalar_prefetch=1,
            grid=(1,),
            in_specs=[pl.BlockSpec(memory_space=pl.ANY)] * (n + 1),
            out_specs=pl.BlockSpec(memory_space=pl.ANY),
            scratch_shapes=[pltpu.VMEM(a.shape, F32) for a in arrived] + [pltpu.SemaphoreType.DMA((n,))] * 2,
        ),
        out_shape=jax.ShapeDtypeStruct(out.shape, F32),
        input_output_aliases={n + 1: 0},
        compiler_params=pltpu.CompilerParams(vmem_limit_bytes=48 * MIB),
        cost_estimate=pl.CostEstimate(flops=5 * 10 ** 9, bytes_accessed=8 * sum(a.size for a in arrived), transcendentals=0),
    )(jnp.concatenate(starts).astype(I32), *arrived, out)


def swap(x, mask, axis="dp"):
    n = 8 if axis == "dp" else 2
    return lax.ppermute(x, axis, [(i, i ^ mask) for i in range(n)])


def solution(mesh):
    n_groups = mesh.shape["dp"]

    def local_step(hidden, mask_pos, labels, w_trans, b_trans, ln_gain, ln_bias, emb_table, b_vocab):
        n_rows, seq_len, width = hidden.shape
        n_masks = mask_pos.shape[1]
        shard_rows = emb_table.shape[0]
        inv_n = 1.0 / (n_rows * n_masks * n_groups)
        n_own = n_rows * SLOTS
        n_all = n_own * n_groups
        me, plane = lax.axis_index("dp"), lax.axis_index("vp")
        core, par = me & 1, ((me >> 1) ^ (me >> 2)) & 1
        row_start = plane * shard_rows
        valid = (jnp.arange(n_own) % SLOTS < n_masks)[None]

        pos = jnp.pad(mask_pos, ((0, 0), (0, SLOTS - n_masks)), constant_values=-1)
        pos_onehot = (pos[:, :, None] == jnp.arange(seq_len)[None, None, :]).astype(BF16)
        masked_h = jnp.einsum("clt,cte->cle", pos_onehot, hidden, preferred_element_type=F32).astype(BF16).reshape(n_own, width)
        pre_act = jnp.dot(masked_h, w_trans, preferred_element_type=F32) + b_trans
        u_norm, head_vjp = jax.vjp(head_norm, pre_act, ln_gain, ln_bias)
        u_own = u_norm.astype(BF16)

        half = n_own // 2
        u_f = u_own.astype(F32)
        u_sib, u_x, u_y = swap(u_f, 1), swap(u_f, 2), swap(u_f, 4)
        u_d0, u_d1 = swap(u_x[:half], 4), swap(u_y[half:], 2)
        u_xs, u_ys = swap(u_x, 1), swap(u_y, 1)
        blk = n_own // 16
        at = lambda m, o=0: ((me ^ m) * blk + o)[None]

        n_steps = -(-shard_rows // VT)
        last = shard_rows - VT
        dup = n_steps * VT - shard_rows
        b_pad = jnp.concatenate([b_vocab[:shard_rows - (VT - dup)], jnp.full((dup,), -OFF, F32), b_vocab[shard_rows - (VT - dup):]]).reshape(n_steps, 1, VT)
        ids = jnp.arange(shard_rows, dtype=F32)
        cols = jnp.concatenate([ids[:shard_rows - (VT - dup)], jnp.full((dup,), -7.0, F32), ids[shard_rows - (VT - dup):]]).reshape(n_steps, 1, VT)
        lab_pad = jnp.pad(labels, ((0, 0), (0, SLOTS - n_masks)), constant_values=-1000000).reshape(n_own)
        lab_rel = (lab_pad - row_start).astype(F32)
        lab_row = lab_rel[None]
        row_block = pl.BlockSpec((1, n_own), lambda i: (0, 0))
        own_block = pl.BlockSpec((n_own, width), lambda i: (0, 0))
        emb_block = pl.BlockSpec((pl.Element(VT), pl.Element(width)), lambda i: (pl.multiple_of(jnp.minimum(i * (VT // 16), last // 16) * 16, 16), 0))
        col_block = pl.BlockSpec((1, 1, VT), lambda i: (i, 0, 0))
        logit_block = pl.BlockSpec((1, n_own, VT), lambda i: (i, 0, 0))
        lane_block = pl.BlockSpec((n_own, 128), lambda i: (0, 0))
        flops = 2 * n_own * shard_rows * width
        cost = pl.CostEstimate(flops=flops, bytes_accessed=4 * n_own * shard_rows, transcendentals=n_own * shard_rows)
        params = pltpu.CompilerParams(vmem_limit_bytes=60 * MIB)
        logits, stats = pl.pallas_call(
            functools.partial(stats_kernel, n_steps),
            grid=(n_steps,),
            in_specs=[own_block, emb_block, col_block, col_block, row_block],
            out_specs=[logit_block, pl.BlockSpec((8, n_own), lambda i: (0, 0))],
            out_shape=[jax.ShapeDtypeStruct((n_steps, n_own, VT), F32), jax.ShapeDtypeStruct((8, n_own), F32)],
            scratch_shapes=[pltpu.VMEM((n_own, 128), F32)] * 4,
            compiler_params=params,
            cost_estimate=cost,
        )(u_own, emb_table, b_pad, cols, lab_row)
        other = swap(stats, 1, "vp")
        lo, hi = jnp.where(plane == 0, stats, other), jnp.where(plane == 0, other, stats)
        top = jnp.maximum(lo[0:1], hi[0:1])
        log_norm = top + jnp.log(lo[1:2] * jnp.exp(lo[0:1] - top) + hi[1:2] * jnp.exp(hi[0:1] - top))
        loss_part = jnp.sum(jnp.where(valid, log_norm - (lo[2:3] + hi[2:3]), 0.0)) * inv_n
        norm_own = jnp.where(valid, log_norm, OFF)

        tok = jnp.concatenate([norm_own, lab_row])
        toks = [tok] + [swap(tok, m) for m in range(1, n_groups)]
        own_du = pl.pallas_call(
            functools.partial(du_kernel, n_steps, inv_n),
            grid=(n_steps,),
            in_specs=[logit_block, emb_block, col_block, row_block, row_block],
            out_specs=[own_block, col_block],
            out_shape=[jax.ShapeDtypeStruct((n_own, width), F32), jax.ShapeDtypeStruct((n_steps, 1, VT), F32)],
            scratch_shapes=[pltpu.VMEM((n_own, width), F32), pltpu.VMEM((n_own, VT), BF16)] + [pltpu.VMEM((n_own, 128), F32)] * 2,
            compiler_params=params,
            cost_estimate=cost,
        )
        du_part, db_tiles = own_du(logits, emb_table, cols, norm_own, lab_row)
        du_other = swap(du_part, 1, "vp")

        (u_d0, u_d1), du_part, db_tiles = lax.optimization_barrier(((u_d0, u_d1), du_part, db_tiles))
        u_ds0, u_ds1 = swap(u_d0, 1), swap(u_d1, 1)
        u_all, = place([u_f, u_sib, u_x, u_y, u_xs, u_ys], jnp.concatenate([at(0), at(1), at(2), at(4), at(3), at(5)]).astype(I32), n_all)
        ranks = [(me ^ m)[None] for m in range(n_groups)]
        (u_all, *toks), du_part, db_tiles = lax.optimization_barrier(((u_all, *toks), du_part, db_tiles))
        u_all, norm_all, lab_all = place(
            [u_d0, u_d1, u_ds0, u_ds1], jnp.concatenate([at(6), at(6, blk // 2), at(7), at(7, blk // 2)] + ranks).astype(I32), n_all, u_all, toks)

        nx, nl = SHARE_CHUNKS * SHARE_TILE // 16, LOCAL_TILES * LOCAL_TILE // 16
        assert 16 * (8 * nx + 2 * nl) == shard_rows
        st = SHARE_TILE // 16
        x_at = lambda p, c, k: ((2 * p + c) * nx + k * st)[None]
        y_at = lambda p, c, k: (4 * nx + (2 * p + c) * nx + k * st)[None]
        pad128 = lambda x: jnp.pad(x, ((0, 0), (0, -x.shape[1] % 128)))[:, None, :]
        bias_share = pad128(b_vocab[:16 * 8 * nx].reshape(-1, SHARE_TILE))
        bias_local = pad128(b_vocab[16 * 8 * nx:].reshape(-1, LOCAL_TILE))
        lt = LOCAL_TILE // 16
        out = None

        def rows_call(out, starts, blocks, bias, tile, n_steps, n_send, take):
            return emb_rows(out, starts, blocks, emb_table, bias, u_all, norm_all, lab_all, inv_n, tile, n_steps, n_send,
                            [a for a, _ in take], [s[:1] for _, s in take])

        per = LOCAL_TILES // LOCAL_CALLS
        l_at = lambda c, k: jnp.stack([8 * nx + c * nl + (k * per + i) * lt for i in range(per)])

        def shared_rows(out, k, take):
            starts = jnp.concatenate([x_at(par, core, k), y_at(par, core, k)])
            return rows_call(out, starts, starts // st, bias_share, SHARE_TILE, 2, 2, take)

        def local_rows(out, k, take):
            starts = l_at(core, k)
            out, rows = rows_call(out, starts, (starts - 8 * nx) // lt, bias_local, LOCAL_TILE, per, 1, take)
            return out, (swap(rows, 1), l_at(1 - core, k))

        def near(k, sx, sy):
            return [(swap(sx, 1), x_at(par, 1 - core, k)), (swap(sy, 1), y_at(par, 1 - core, k))]

        def far(k, rx, ry):
            return [(rx, x_at(1 - par, core, k)), (ry, y_at(1 - par, core, k)),
                    (swap(rx, 1), x_at(1 - par, 1 - core, k)),
                    (swap(ry, 1), y_at(1 - par, 1 - core, k))]

        after = lax.optimization_barrier
        out, sx0, sy0 = shared_rows(out, 0, [])
        rx0, ry0 = swap(sx0, 2), swap(sy0, 4)
        near0 = near(0, sx0, sy0)
        out, sx1, sy1 = shared_rows(out, 1, [])
        rx1, ry1 = swap(sx1, 2), swap(sy1, 4)
        near1 = near(1, sx1, sy1)

        du_other, out = after((du_other, out))
        d_pre, d_ln_gain, d_ln_bias = head_vjp(du_part + du_other)
        d_pre_bf = d_pre.astype(BF16)
        d_w_part = lax.dot_general(masked_h, d_pre_bf, (((0,), (0,)), ((), ())), preferred_element_type=F32)
        hw = width // 2
        db_flat = db_tiles.reshape(n_steps * VT)
        db_own = jnp.concatenate([db_flat[:shard_rows - (VT - dup)], db_flat[shard_rows - (VT - dup) + dup:]])
        db_rows = -(-shard_rows // width)
        small = jnp.concatenate([jnp.sum(d_pre, axis=0), d_ln_gain, d_ln_bias, jnp.pad(loss_part[None], (0, width - 1)),
                                 jnp.pad(db_own, (0, db_rows * width - shard_rows))]).reshape(4 + db_rows, width)
        total = hw + 4 + db_rows
        padded = -(-total // 64) * 64
        part = padded // n_groups
        mine = jnp.concatenate([lax.dynamic_slice(d_w_part, (plane * hw, 0), (hw, width)), small, jnp.zeros((padded - total, width), F32)])
        mine = mine.reshape(n_groups, part, width)
        mine, out, d_pre_bf = after((mine, out, d_pre_bf))
        piece = lambda a, m: lax.dynamic_index_in_dim(a, me ^ m, 0, keepdims=False)
        got = [swap(piece(mine, m), m) for m in range(1, n_groups)]

        out, sx2, sy2 = shared_rows(out, 2, [])
        near2 = near(2, sx2, sy2)
        out, sx3, sy3 = shared_rows(out, 3, [])
        near3 = near(3, sx3, sy3)
        out, rx0, ry0, sx2, sy2 = after((out, rx0, ry0, sx2, sy2))
        rx2, ry2 = swap(sx2, 2), swap(sy2, 4)
        far0 = far(0, rx0, ry0)
        d_masked = dot_nt(d_pre_bf, w_trans).astype(BF16).reshape(n_rows, SLOTS, width)
        out, got0 = local_rows(out, 0, near0 + near1 + near2)
        out, got, d_masked = after((out, got, d_masked))
        parts = [piece(mine, 0)] + got
        order = [parts[m] for m in range(n_groups)]
        level = lambda v: [v[i] + v[i + 1] for i in range(0, len(v), 2)]
        acc = level(level(level(order)))[0]
        acc, out = after((acc, out))
        sums = [acc] + [swap(acc, m) for m in range(1, n_groups)]
        out, got1 = local_rows(out, 1, near3 + far0)
        out, rx1, ry1, sx3, sy3 = after((out, rx1, ry1, sx3, sy3))
        rx3, ry3 = swap(sx3, 2), swap(sy3, 4)
        far1 = far(1, rx1, ry1)
        (sums, out) = after((sums, out))
        grads = jnp.zeros((n_groups, part, width), F32)
        for m in range(n_groups):
            grads = lax.dynamic_update_index_in_dim(grads, sums[m], me ^ m, 0)
        grads = grads.reshape(padded, width)
        w_other = swap(grads[:hw], 1, "vp")
        out, got2 = local_rows(out, 2, far1[:2] + [got0])
        d_hidden = jnp.einsum("clt,cle->cte", pos_onehot, d_masked, preferred_element_type=F32).astype(BF16)
        out, rx2, ry2, d_hidden = after((out, rx2, ry2, d_hidden))
        far2 = far(2, rx2, ry2)
        put = lambda out, items: copy_rows(out, [a for a, _ in items], [s[:1] for _, s in items])
        out = put(out, far1[2:] + [got1, got2] + far2)
        out, rx3, ry3 = after((out, rx3, ry3))
        far3 = far(3, rx3, ry3)
        d_emb_table = put(out, far3)
        w_half = grads[:hw]
        d_w_trans = jnp.where(plane == 0, jnp.concatenate([w_half, w_other]), jnp.concatenate([w_other, w_half]))
        vec = grads[hw:hw + 3]
        mlm_loss = grads[hw + 3, 0]
        d_b_vocab = grads[hw + 4:total].reshape(db_rows * width)[:shard_rows]
        return mlm_loss, d_hidden, d_w_trans, vec[0], vec[1], vec[2], d_emb_table, d_b_vocab

    in_specs = (P("dp", None, None), P("dp", None), P("dp", None), P(None, None), P(None), P(None), P(None), P("vp", None), P("vp"))
    out_specs = (P(), P("dp", None, None), P(None, None), P(None), P(None), P(None), P("vp", None), P("vp"))

    return jax.shard_map(local_step, mesh=mesh, in_specs=in_specs, out_specs=out_specs, check_vma=False)
```

```python
import functools

import jax
import jax.numpy as jnp
from jax import lax
from jax.experimental import pallas as pl
from jax.experimental.pallas import tpu as pltpu
from jax.sharding import PartitionSpec as P


LN_EPS = 1e-5

BF16, F32, I32 = jnp.bfloat16, jnp.float32, jnp.int32
SLOTS = 80
OWN_SPLIT = 7
VT = 2304
CHUNK = 768
SHARE_CHUNKS, SHARE_TILE = 4, 624
LOCAL_TILES, LOCAL_TILE = 6, 432
LOCAL_CALLS = 2
TOK_CHUNK = 1280
VMEM_ROWS = 44
COST_SCALE = 4
OFF = 1e30
MIB = 2 ** 20


def head_norm(pre_act, ln_gain, ln_bias):
    gelu_out = jax.nn.gelu(pre_act, approximate=False)
    row_mean = jnp.mean(gelu_out, axis=-1, keepdims=True)
    centered = gelu_out - row_mean
    row_var = jnp.mean(centered * centered, axis=-1, keepdims=True)
    return centered * lax.rsqrt(row_var + LN_EPS) * ln_gain + ln_bias


def dot_nt(a, b):
    return lax.dot_general(a, b, (((1,), (1,)), ((), ())), preferred_element_type=F32)


def to_lanes(row):
    return jnp.broadcast_to(row, (128, row.shape[1])).T


def front_kernel(n_steps, hid_ref, pos_ref, w_ref, vec_ref, z_ref, pre_ref, u_ref, uf_ref):
    step = pl.program_id(0)
    pos = to_lanes(pos_ref[0])[:SLOTS]
    lane = lax.broadcasted_iota(I32, (SLOTS, 128), 1).astype(F32)
    hot = jnp.concatenate([jnp.where(pos == lane + k * 128.0, 1.0, 0.0) for k in range(hid_ref.shape[1] // 128)], axis=1)
    rows = pl.ds(pl.multiple_of(step * SLOTS, 16), SLOTS)
    z_ref[rows, :] = jnp.dot(hot.astype(BF16), hid_ref[0], preferred_element_type=F32).astype(BF16)

    @pl.when(step == n_steps - 1)
    def _():
        pre = jnp.dot(z_ref[...], w_ref[...], preferred_element_type=F32) + vec_ref[0:1, :]
        pre_ref[...] = pre
        act = 0.5 * pre * (1.0 + lax.erf(pre * 0.7071067811865476))
        cen = act - jnp.mean(act, axis=1, keepdims=True)
        var = jnp.mean(cen * cen, axis=1, keepdims=True)
        u = (cen * lax.rsqrt(var + LN_EPS) * vec_ref[1:2, :] + vec_ref[2:3, :]).astype(BF16)
        u_ref[...] = u
        uf_ref[...] = u.astype(F32)


def own_kernel(n_steps, first, u_ref, emb_ref, bias_ref, col_ref, lab_row_ref, *refs):
    acc_in, state_in = (None, None) if first else refs[:2]
    acc_ref, stat_ref, m_ref, s_ref, t_ref, lab_ref = refs if first else refs[2:]
    step = pl.program_id(0)

    @pl.when(step == 0)
    def _():
        lab_ref[...] = to_lanes(lab_row_ref[...])
        if first:
            m_ref[...] = jnp.full_like(m_ref, -1e38)
            s_ref[...] = jnp.zeros_like(s_ref)
            t_ref[...] = jnp.zeros_like(t_ref)
            acc_ref[...] = jnp.zeros_like(acc_ref)
        else:
            m_ref[...], s_ref[...], t_ref[...] = state_in[0], state_in[1], state_in[2]
            acc_ref[...] = acc_in[...]

    wide = lambda x, n: jnp.concatenate([x] * (n // 128), axis=1)
    fold = lambda x: functools.reduce(jnp.add, [x[:, k * 128:(k + 1) * 128] for k in range(CHUNK // 128)])
    logit = lambda q: dot_nt(u_ref[...], emb_ref[q * CHUNK:(q + 1) * CHUNK, :]) + bias_ref[0, :, q * CHUNK:(q + 1) * CHUNK]
    following = logit(0)
    for q in range(VT // CHUNK):
        block, cs = following, slice(q * CHUNK, (q + 1) * CHUNK)
        if q + 1 < VT // CHUNK:
            following = logit(q + 1)
        hot = col_ref[0, :, cs] == wide(lab_ref[...], CHUNK)
        m_old = m_ref[...]
        m_new = jnp.maximum(m_old, jnp.max(block, axis=1, keepdims=True))
        scale = jnp.exp(m_old - m_new)
        prob = jnp.exp(block - wide(m_new, CHUNK))
        m_ref[...] = m_new
        s_ref[...] = s_ref[...] * scale + fold(prob)
        t_ref[...] += fold(jnp.where(hot, block, 0.0))
        rest = jnp.where(hot, 0.0, prob).astype(BF16)
        acc_ref[...] = acc_ref[...] * wide(scale, acc_ref.shape[1]) + jnp.dot(rest, emb_ref[cs, :], preferred_element_type=F32)

    @pl.when(step == n_steps - 1)
    def _():
        if first:
            for k, ref in enumerate((m_ref, s_ref, t_ref)):
                stat_ref[k] = ref[...]
            return
        mass = jnp.sum(s_ref[...], axis=1, keepdims=True)
        target = jnp.sum(t_ref[...], axis=1, keepdims=True)
        lane = lax.broadcasted_iota(I32, m_ref.shape, 1)
        stat_ref[...] = jnp.where(lane == 0, m_ref[...], jnp.where(lane == 1, mass, target)).T[:8]


def norm_kernel(n_masks, inv_n, shard_rows, plane_ref, mine_ref, other_ref, lab_ref, tok_ref, coef_ref, loss_ref):
    low = plane_ref[0] == 0
    mine, other = mine_ref[...], other_ref[...]
    lo, hi = jnp.where(low, mine, other), jnp.where(low, other, mine)
    top = jnp.maximum(lo[0:1], hi[0:1])
    log_norm = top + jnp.log(lo[1:2] * jnp.exp(lo[0:1] - top) + hi[1:2] * jnp.exp(hi[0:1] - top))
    valid = lax.rem(lax.broadcasted_iota(I32, log_norm.shape, 1), SLOTS) < n_masks
    norm = jnp.where(valid, log_norm, OFF)
    lab = lab_ref[...]
    tok_ref[0:1, :] = norm
    tok_ref[1:2, :] = lab
    here = (lab >= 0.0) & (lab < shard_rows)
    coef_ref[0:1, :] = jnp.exp(mine[0:1] - norm) * inv_n
    coef_ref[1:2, :] = jnp.where(here, (jnp.exp(mine[2:3] - norm) - 1.0) * inv_n, 0.0)
    loss = jnp.sum(jnp.where(valid, log_norm - (lo[2:3] + hi[2:3]), 0.0), axis=1, keepdims=True) * inv_n
    loss_ref[...] = jnp.broadcast_to(loss, loss_ref.shape)


def du_kernel(acc_ref, row_ref, coef_ref, du_ref):
    wide = lambda x: jnp.concatenate([x] * (acc_ref.shape[1] // 128), axis=1)
    hot = to_lanes(coef_ref[1:2, :]).astype(BF16).astype(F32)
    du = acc_ref[...] * wide(to_lanes(coef_ref[0:1, :])) + row_ref[...].astype(F32) * wide(hot)
    du_ref[...] = du.astype(BF16).astype(F32)


def place_kernel(n, start_ref, *refs):
    pieces, out_ref, bufs, sems = refs[:n], refs[n], refs[n + 1:-1], refs[-1]
    loads = [pltpu.make_async_copy(pieces[k], bufs[k], sems.at[k]) for k in range(n)]
    for load in loads:
        load.start()
    for k in range(n):
        loads[k].wait()
        out_ref[pl.ds(pl.multiple_of(start_ref[k] * 16, 16), pieces[k].shape[0]), :] = bufs[k][...].astype(BF16)


def place(pieces, starts, n_all):
    n, width = len(pieces), pieces[0].shape[1]
    return pl.pallas_call(
        functools.partial(place_kernel, n),
        grid_spec=pltpu.PrefetchScalarGridSpec(
            num_scalar_prefetch=1,
            grid=(1,),
            in_specs=[pl.BlockSpec(memory_space=pl.ANY)] * n,
            out_specs=pl.BlockSpec(memory_space=pltpu.VMEM),
            scratch_shapes=[pltpu.VMEM(p.shape, F32) for p in pieces] + [pltpu.SemaphoreType.DMA((n,))],
        ),
        out_shape=jax.ShapeDtypeStruct((n_all, width), BF16),
        compiler_params=pltpu.CompilerParams(vmem_limit_bytes=40 * MIB),
        cost_estimate=pl.CostEstimate(flops=5 * 10 ** 9, bytes_accessed=6 * n_all * width, transcendentals=0),
    )(starts, *pieces)


def tok_kernel(n, start_ref, *refs):
    for k in range(n):
        row = pl.ds(start_ref[k], 1)
        refs[n][row, :] = refs[k][0:1, :]
        refs[n + 1][row, :] = refs[k][1:2, :]


def place_toks(toks, ranks):
    n, width = len(toks), toks[0].shape[1]
    return pl.pallas_call(
        functools.partial(tok_kernel, n),
        grid_spec=pltpu.PrefetchScalarGridSpec(
            num_scalar_prefetch=1,
            grid=(1,),
            in_specs=[pl.BlockSpec(t.shape, lambda i, s: (0, 0)) for t in toks],
            out_specs=[pl.BlockSpec((n, width), lambda i, s: (0, 0))] * 2,
        ),
        out_shape=[jax.ShapeDtypeStruct((n, width), F32)] * 2,
    )(ranks, *toks)


def piece_kernel(n, start_ref, *refs):
    for k in range(n):
        refs[n][start_ref[k]] = refs[k][...]


def gather_pieces(pieces, ranks):
    n = len(pieces)
    shape = (n,) + pieces[0].shape
    return pl.pallas_call(
        functools.partial(piece_kernel, n),
        grid_spec=pltpu.PrefetchScalarGridSpec(
            num_scalar_prefetch=1,
            grid=(1,),
            in_specs=[pl.BlockSpec(p.shape, lambda i, s: (0, 0)) for p in pieces],
            out_specs=pl.BlockSpec(shape, lambda i, s: (0, 0, 0)),
        ),
        out_shape=jax.ShapeDtypeStruct(shape, F32),
    )(ranks, *pieces)


def rows_kernel(cfg, start_ref, emb_ref, bias_ref, u_ref, norm_ref, lab_ref, *refs):
    n_steps, tile, inv_n, n_send, n_copy, aliased = cfg
    arrived, refs = refs[:n_copy], refs[n_copy + (1 if aliased else 0):]
    out_ref, db_ref, sends, refs = refs[0], refs[1], refs[2:2 + n_send], refs[2 + n_send:]
    acc_ref, out_sem, send_sem = refs[:3]
    stage, load_sem, store_sem = (refs[3:3 + n_copy], refs[3 + n_copy], refs[4 + n_copy]) if n_copy else ((), None, None)
    step = pl.program_id(0)
    slot = lax.rem(step, 2)
    n_tok = u_ref.shape[0]

    def load(k):
        return pltpu.make_async_copy(arrived[k], stage[k], load_sem.at[k])

    def store(k):
        rows = pl.ds(pl.multiple_of(start_ref[2 * n_steps + k] * 16, 16), arrived[k].shape[0])
        return pltpu.make_async_copy(stage[k], out_ref.at[rows, :], store_sem.at[k])

    @pl.when(step == 0)
    def _():
        for k in range(n_copy):
            load(k).start()

    @pl.when(step == 1)
    def _():
        for k in range(n_copy):
            load(k).wait()
            store(k).start()

    def out_copy(t, which):
        rows = pl.ds(pl.multiple_of(start_ref[t] * 16, 16), tile)
        return pltpu.make_async_copy(acc_ref.at[which], out_ref.at[rows, :], out_sem.at[which])

    def send_copy(t, which):
        rows = pl.ds(pl.multiple_of(t * tile, 16), tile) if n_send == 1 else pl.ds(0, tile)
        target = sends[0] if n_send == 1 else sends[t]
        return pltpu.make_async_copy(acc_ref.at[which], target.at[rows, :], send_sem.at[which])

    @pl.when(step >= 2)
    def _():
        out_copy(step - 2, slot).wait()
        pltpu.make_async_copy(acc_ref.at[slot], sends[0].at[pl.ds(0, tile), :], send_sem.at[slot]).wait()

    row_id = lax.broadcasted_iota(I32, (tile, 1), 0).astype(F32) + (start_ref[step] * 16).astype(F32)
    bias = jnp.concatenate([to_lanes(bias_ref[0])[:tile]] * (TOK_CHUNK // 128), axis=1)
    per = TOK_CHUNK // norm_ref.shape[1]
    for j in range(n_tok // TOK_CHUNK):
        s = slice(j * TOK_CHUNK, (j + 1) * TOK_CHUNK)
        norm = jnp.concatenate([norm_ref[i:i + 1, :] for i in range(j * per, (j + 1) * per)], axis=1)
        lab = jnp.concatenate([lab_ref[i:i + 1, :] for i in range(j * per, (j + 1) * per)], axis=1)
        logit = dot_nt(emb_ref[...], u_ref[s, :]) + bias
        prob = jnp.exp(logit - norm)
        grad = (prob - jnp.where(lab == row_id, 1.0, 0.0)) * inv_n
        part = jnp.dot(grad.astype(BF16), u_ref[s, :], preferred_element_type=F32)
        lanes = functools.reduce(jnp.add, [grad[:, k * 128:(k + 1) * 128] for k in range(TOK_CHUNK // 128)])
        db = lanes if j == 0 else db + lanes
        if j == 0:
            acc_ref[slot] = part
        else:
            acc_ref[slot] += part

    db = jnp.concatenate([db, jnp.zeros((db_ref.shape[2] - tile, 128), F32)])
    db_ref[0] = jnp.sum(db.T, axis=0, keepdims=True)
    out_copy(step, slot).start()
    if n_send == 1:
        send_copy(step, slot).start()
    else:
        for t in range(n_send):
            @pl.when(step == t)
            def _():
                send_copy(t, t % 2).start()

    @pl.when(step == n_steps - 1)
    def _():
        for k in range(n_copy):
            store(k).wait()
        for t in range(max(0, n_steps - 2), n_steps):
            out_copy(t, t % 2).wait()
            pltpu.make_async_copy(acc_ref.at[t % 2], sends[0].at[pl.ds(0, tile), :], send_sem.at[t % 2]).wait()


def emb_rows(out, starts, blocks, emb, bias, u_all, norm, lab, inv_n, tile, n_steps, n_send, arrived, copy_starts):
    n_tok, width = u_all.shape
    n_rows = emb.shape[0]
    n_copy = len(arrived)
    aliased = out is not None
    cfg = (n_steps, tile, inv_n, n_send, n_copy, aliased)
    table = jnp.concatenate([starts, blocks] + list(copy_starts)).astype(I32)
    any_space = pl.BlockSpec(memory_space=pl.ANY)
    whole = lambda a: pl.BlockSpec(a.shape, lambda i, s: (0, 0))
    send_rows = n_steps * tile if n_send == 1 else tile
    scratch = [pltpu.VMEM((2, tile, width), F32), pltpu.SemaphoreType.DMA((2,)), pltpu.SemaphoreType.DMA((2,))]
    if n_copy:
        scratch += [pltpu.VMEM(a.shape, F32) for a in arrived] + [pltpu.SemaphoreType.DMA((n_copy,))] * 2
    return pl.pallas_call(
        functools.partial(rows_kernel, cfg),
        grid_spec=pltpu.PrefetchScalarGridSpec(
            num_scalar_prefetch=1,
            grid=(n_steps,),
            in_specs=[
                pl.BlockSpec((pl.Element(tile), pl.Element(width)), lambda i, s: (pl.multiple_of(s[i] * 16, 16), 0)),
                pl.BlockSpec((1, 1, bias.shape[2]), lambda i, s: (s[n_steps + i], 0, 0)),
                pl.BlockSpec(memory_space=pltpu.VMEM), whole(norm), whole(lab),
            ] + [any_space] * (n_copy + aliased),
            out_specs=[any_space, pl.BlockSpec((1, 1, bias.shape[2]), lambda i, s: (i, 0, 0))] + [any_space] * n_send,
            scratch_shapes=scratch,
        ),
        out_shape=[jax.ShapeDtypeStruct((n_rows, width), F32), jax.ShapeDtypeStruct((n_steps, 1, bias.shape[2]), F32)] + [jax.ShapeDtypeStruct((send_rows, width), F32)] * n_send,
        input_output_aliases={6 + n_copy: 0} if aliased else {},
        compiler_params=pltpu.CompilerParams(vmem_limit_bytes=VMEM_ROWS * MIB),
        cost_estimate=pl.CostEstimate(
            flops=n_steps * tile * n_tok * width // COST_SCALE, bytes_accessed=n_steps * tile * width * 10, transcendentals=n_steps * tile * n_tok
        ),
    )(table, emb, bias, u_all, norm, lab, *arrived, *([out] if aliased else []))


def copy_kernel(n, start_ref, *refs):
    arrived, out_ref, stage, load_sem, store_sem = refs[:n], refs[n + 1], refs[n + 2:-2], refs[-2], refs[-1]
    loads = [pltpu.make_async_copy(arrived[k], stage[k], load_sem.at[k]) for k in range(n)]
    for load in loads:
        load.start()
    stores = []
    for k in range(n):
        loads[k].wait()
        rows = pl.ds(pl.multiple_of(start_ref[k] * 16, 16), arrived[k].shape[0])
        stores.append(pltpu.make_async_copy(stage[k], out_ref.at[rows, :], store_sem.at[k]))
        stores[-1].start()
    for store in stores:
        store.wait()


def copy_rows(out, arrived, starts):
    n = len(arrived)
    return pl.pallas_call(
        functools.partial(copy_kernel, n),
        grid_spec=pltpu.PrefetchScalarGridSpec(
            num_scalar_prefetch=1,
            grid=(1,),
            in_specs=[pl.BlockSpec(memory_space=pl.ANY)] * (n + 1),
            out_specs=pl.BlockSpec(memory_space=pl.ANY),
            scratch_shapes=[pltpu.VMEM(a.shape, F32) for a in arrived] + [pltpu.SemaphoreType.DMA((n,))] * 2,
        ),
        out_shape=jax.ShapeDtypeStruct(out.shape, F32),
        input_output_aliases={n + 1: 0},
        compiler_params=pltpu.CompilerParams(vmem_limit_bytes=48 * MIB),
        cost_estimate=pl.CostEstimate(flops=5 * 10 ** 9, bytes_accessed=8 * sum(a.size for a in arrived), transcendentals=0),
    )(jnp.concatenate(starts).astype(I32), *arrived, out)


def swap(x, mask, axis="dp"):
    n = 8 if axis == "dp" else 2
    return lax.ppermute(x, axis, [(i, i ^ mask) for i in range(n)])


def solution(mesh):
    n_groups = mesh.shape["dp"]

    def local_step(hidden, mask_pos, labels, w_trans, b_trans, ln_gain, ln_bias, emb_table, b_vocab):
        n_rows, seq_len, width = hidden.shape
        n_masks = mask_pos.shape[1]
        shard_rows = emb_table.shape[0]
        inv_n = 1.0 / (n_rows * n_masks * n_groups)
        n_own = n_rows * SLOTS
        n_all = n_own * n_groups
        me, plane = lax.axis_index("dp"), lax.axis_index("vp")
        core, par = me & 1, ((me >> 1) ^ (me >> 2)) & 1
        row_start = plane * shard_rows

        pos = jnp.pad(mask_pos, ((0, 0), (0, SLOTS - n_masks)), constant_values=-1)
        pos_onehot = (pos[:, :, None] == jnp.arange(seq_len)[None, None, :]).astype(BF16)
        pos_row = jnp.pad(mask_pos, ((0, 0), (0, 128 - n_masks)), constant_values=-1).astype(F32)[:, None, :]
        tok_f32, tok_bf16 = jax.ShapeDtypeStruct((n_own, width), F32), jax.ShapeDtypeStruct((n_own, width), BF16)
        own_block = pl.BlockSpec((n_own, width), lambda i: (0, 0))
        masked_h, pre_act, u_own, u_f = pl.pallas_call(
            functools.partial(front_kernel, n_rows),
            grid=(n_rows,),
            in_specs=[
                pl.BlockSpec((1, seq_len, width), lambda i: (i, 0, 0)), pl.BlockSpec((1, 1, 128), lambda i: (i, 0, 0)),
                pl.BlockSpec((width, width), lambda i: (0, 0)), pl.BlockSpec((3, width), lambda i: (0, 0)),
            ],
            out_specs=[own_block] * 4,
            out_shape=[tok_bf16, tok_f32, tok_bf16, tok_f32],
            compiler_params=pltpu.CompilerParams(vmem_limit_bytes=48 * MIB),
            cost_estimate=pl.CostEstimate(flops=2 * n_own * width * (width + seq_len), bytes_accessed=2 * hidden.size, transcendentals=0),
        )(hidden, pos_row, w_trans, jnp.stack([b_trans, ln_gain, ln_bias]))

        _, head_vjp = jax.vjp(head_norm, pre_act, ln_gain, ln_bias)

        half = n_own // 2
        u_sib, u_x, u_y = swap(u_f, 1), swap(u_f, 2), swap(u_f, 4)
        blk = n_own // 16
        at = lambda m, o=0: ((me ^ m) * blk + o)[None]

        n_steps = -(-shard_rows // VT)
        last = shard_rows - VT
        dup = n_steps * VT - shard_rows
        b_pad = jnp.concatenate([b_vocab[:shard_rows - (VT - dup)], jnp.full((dup,), -OFF, F32), b_vocab[shard_rows - (VT - dup):]]).reshape(n_steps, 1, VT)
        ids = jnp.arange(shard_rows, dtype=F32)
        cols = jnp.concatenate([ids[:shard_rows - (VT - dup)], jnp.full((dup,), -7.0, F32), ids[shard_rows - (VT - dup):]]).reshape(n_steps, 1, VT)
        lab_pad = jnp.pad(labels, ((0, 0), (0, SLOTS - n_masks)), constant_values=-1000000).reshape(n_own)
        lab_rel = (lab_pad - row_start).astype(F32)
        lab_row = lab_rel[None]
        row_block = pl.BlockSpec((1, n_own), lambda i: (0, 0))
        emb_block = pl.BlockSpec((pl.Element(VT), pl.Element(width)), lambda i: (pl.multiple_of(jnp.minimum(i * (VT // 16), last // 16) * 16, 16), 0))
        col_block = pl.BlockSpec((1, 1, VT), lambda i: (i, 0, 0))
        state = jax.ShapeDtypeStruct((3, n_own, 128), F32)
        state_block = pl.BlockSpec(state.shape, lambda i: (0, 0, 0))

        def own_call(begin, end, carry):
            first = not carry
            skip = lambda i: i + begin
            last_shape = state if first else jax.ShapeDtypeStruct((8, n_own), F32)
            return pl.pallas_call(
                functools.partial(own_kernel, end - begin, first),
                grid=(end - begin,),
                in_specs=[
                    own_block,
                    pl.BlockSpec((pl.Element(VT), pl.Element(width)), lambda i: (pl.multiple_of(jnp.minimum(skip(i) * (VT // 16), last // 16) * 16, 16), 0)),
                    pl.BlockSpec((1, 1, VT), lambda i: (skip(i), 0, 0)), pl.BlockSpec((1, 1, VT), lambda i: (skip(i), 0, 0)), row_block,
                ] + ([] if first else [own_block, state_block]),
                out_specs=[own_block, state_block if first else pl.BlockSpec((8, n_own), lambda i: (0, 0))],
                out_shape=[tok_f32, last_shape],
                scratch_shapes=[pltpu.VMEM((n_own, 128), F32)] * 4,
                compiler_params=pltpu.CompilerParams(vmem_limit_bytes=56 * MIB),
                cost_estimate=pl.CostEstimate(
                    flops=4 * n_own * (end - begin) * VT * width // COST_SCALE, bytes_accessed=2 * (end - begin) * VT * width, transcendentals=n_own * shard_rows),
            )(u_own, emb_table, b_pad, cols, lab_row, *carry)

        carry = own_call(0, OWN_SPLIT, ())
        u_x, u_y, carry = lax.optimization_barrier((u_x, u_y, carry))
        u_d0, u_d1 = swap(u_x[:half], 4), swap(u_y[half:], 2)
        u_xs, u_ys = swap(u_x, 1), swap(u_y, 1)
        du_sum, stats = own_call(OWN_SPLIT, n_steps, carry)
        lab_local = lab_pad - row_start
        spread = jnp.arange(n_own, dtype=I32) * (shard_rows // n_own)
        label_rows = jnp.take(emb_table, jnp.where((lab_local >= 0) & (lab_local < shard_rows), lab_local, spread), axis=0)
        other = swap(stats, 1, "vp")
        (u_d0, u_d1), du_sum = lax.optimization_barrier(((u_d0, u_d1), du_sum))
        u_ds0, u_ds1 = swap(u_d0, 1), swap(u_d1, 1)

        u_all = place(
            [u_f, u_sib, u_x, u_y, u_xs, u_ys, u_d0, u_d1, u_ds0, u_ds1],
            jnp.concatenate([at(0), at(1), at(2), at(4), at(3), at(5), at(6), at(6, blk // 2), at(7), at(7, blk // 2)]).astype(I32), n_all)
        tok, coef, loss_row = pl.pallas_call(
            functools.partial(norm_kernel, n_masks, inv_n, shard_rows),
            in_specs=[pl.BlockSpec(memory_space=pltpu.SMEM)] + [pl.BlockSpec(memory_space=pltpu.VMEM)] * 3,
            out_shape=[jax.ShapeDtypeStruct((2, n_own), F32)] * 2 + [jax.ShapeDtypeStruct((1, width), F32)],
        )(plane[None], stats, other, lab_row)
        toks = [tok] + [swap(tok, m) for m in range(1, n_groups)]
        du_part = pl.pallas_call(
            du_kernel, out_shape=tok_f32, compiler_params=pltpu.CompilerParams(vmem_limit_bytes=32 * MIB),
            cost_estimate=pl.CostEstimate(flops=10 ** 9, bytes_accessed=10 * n_own * width, transcendentals=0),
        )(du_sum, label_rows, coef)
        du_other = swap(du_part, 1, "vp")
        ranks = jnp.stack([me ^ m for m in range(n_groups)]).astype(I32)
        norm_all, lab_all = place_toks(toks, ranks)

        nx, nl = SHARE_CHUNKS * SHARE_TILE // 16, LOCAL_TILES * LOCAL_TILE // 16
        assert 16 * (8 * nx + 2 * nl) == shard_rows
        st = SHARE_TILE // 16
        x_at = lambda p, c, k: ((2 * p + c) * nx + k * st)[None]
        y_at = lambda p, c, k: (4 * nx + (2 * p + c) * nx + k * st)[None]
        pad128 = lambda x: jnp.pad(x, ((0, 0), (0, -x.shape[1] % 128)))[:, None, :]
        bias_share = pad128(b_vocab[:16 * 8 * nx].reshape(-1, SHARE_TILE))
        bias_local = pad128(b_vocab[16 * 8 * nx:].reshape(-1, LOCAL_TILE))
        lt = LOCAL_TILE // 16
        out = None

        def rows_call(out, starts, blocks, bias, tile, n_steps, n_send, take):
            return emb_rows(out, starts, blocks, emb_table, bias, u_all, norm_all, lab_all, inv_n, tile, n_steps, n_send,
                            [a for a, _ in take], [s[:1] for _, s in take])

        per = LOCAL_TILES // LOCAL_CALLS
        l_at = lambda c, k: jnp.stack([8 * nx + c * nl + (k * per + i) * lt for i in range(per)])

        def shared_rows(out, k, take):
            starts = jnp.concatenate([x_at(par, core, k), y_at(par, core, k)])
            return rows_call(out, starts, starts // st, bias_share, SHARE_TILE, 2, 2, take)

        def local_rows(out, k, take):
            starts = l_at(core, k)
            out, db, rows = rows_call(out, starts, (starts - 8 * nx) // lt, bias_local, LOCAL_TILE, per, 1, take)
            return out, (swap(rows, 1), l_at(1 - core, k)), db[:, 0, :LOCAL_TILE]

        def near(k, sx, sy):
            return [(swap(sx, 1), x_at(par, 1 - core, k)), (swap(sy, 1), y_at(par, 1 - core, k))]

        def far(k, rx, ry):
            return [(rx, x_at(1 - par, core, k)), (ry, y_at(1 - par, core, k)),
                    (swap(rx, 1), x_at(1 - par, 1 - core, k)),
                    (swap(ry, 1), y_at(1 - par, 1 - core, k))]

        after = lax.optimization_barrier
        out, db0, sx0, sy0 = shared_rows(out, 0, [])
        rx0, ry0 = swap(sx0, 2), swap(sy0, 4)
        near0 = near(0, sx0, sy0)
        out, db1, sx1, sy1 = shared_rows(out, 1, [])
        rx1, ry1 = swap(sx1, 2), swap(sy1, 4)
        near1 = near(1, sx1, sy1)

        du_other, out = after((du_other, out))
        d_pre, d_ln_gain, d_ln_bias = head_vjp(du_part + du_other)
        d_pre_bf = d_pre.astype(BF16)
        d_w_part = lax.dot_general(masked_h, d_pre_bf, (((0,), (0,)), ((), ())), preferred_element_type=F32)
        hw = width // 2
        small = jnp.concatenate([jnp.sum(d_pre, axis=0), d_ln_gain, d_ln_bias, loss_row[0]]).reshape(4, width)
        total = hw + 4
        padded = -(-total // 64) * 64
        part = padded // n_groups
        mine = jnp.concatenate([lax.dynamic_slice(d_w_part, (plane * hw, 0), (hw, width)), small, jnp.zeros((padded - total, width), F32)])
        mine = mine.reshape(n_groups, part, width)
        mine, out, d_pre_bf = after((mine, out, d_pre_bf))
        piece = lambda a, m: lax.dynamic_index_in_dim(a, me ^ m, 0, keepdims=False)
        got = [swap(piece(mine, m), m) for m in range(1, n_groups)]

        out, db2, sx2, sy2 = shared_rows(out, 2, [])
        near2 = near(2, sx2, sy2)
        out, rx0, ry0, sx2, sy2 = after((out, rx0, ry0, sx2, sy2))
        rx2, ry2 = swap(sx2, 2), swap(sy2, 4)
        far0 = far(0, rx0, ry0)
        out, db3, sx3, sy3 = shared_rows(out, 3, near0 + near1)
        near3 = near(3, sx3, sy3)
        out, rx1, ry1, sx3, sy3, got = after((out, rx1, ry1, sx3, sy3, got))
        rx3, ry3 = swap(sx3, 2), swap(sy3, 4)
        far1 = far(1, rx1, ry1)
        parts = [piece(mine, 0)] + got
        level = lambda v: [v[i] + v[i + 1] for i in range(0, len(v), 2)]
        acc = level(level(level(parts)))[0]
        db_mine = jnp.stack([jnp.concatenate([d[i, 0, :SHARE_TILE] for d in (db0, db1, db2, db3)]) for i in range(2)])
        acc, db_mine, out = after((acc, db_mine, out))
        sums = [acc] + [swap(acc, m) for m in range(1, n_groups)]
        db_rel = [db_mine] + [swap(db_mine, m) for m in (1, 2, 3)]
        out, got0, dl0 = local_rows(out, 0, near2 + far0)
        sums, out = after((sums, out))
        grads = gather_pieces(sums, ranks).reshape(padded, width)
        w_half, out = after((grads[:hw], out))
        w_other = swap(w_half, 1, "vp")
        d_masked = dot_nt(d_pre_bf, w_trans).astype(BF16).reshape(n_rows, SLOTS, width)
        out, rx2, ry2, d_masked, db_rel = after((out, rx2, ry2, d_masked, db_rel))
        far2 = far(2, rx2, ry2)
        db_sh = jnp.stack(db_rel, 1).reshape(2, 2, 2, 16 * nx)
        db_sh = jnp.where(par == 1, jnp.flip(db_sh, 1), db_sh)
        db_sh = jnp.where(core == 1, jnp.flip(db_sh, 2), db_sh).reshape(2 * 4 * 16 * nx)
        out, got1, dl1 = local_rows(out, 1, near3 + far1 + far2[:2])
        out, rx3, ry3 = after((out, rx3, ry3))
        far3 = far(3, rx3, ry3)
        dl_mine = jnp.concatenate([dl0, dl1]).reshape(16 * nl)
        dl_other = swap(dl_mine, 1)
        d_hidden = jnp.einsum("clt,cle->cte", pos_onehot, d_masked, preferred_element_type=F32).astype(BF16)
        put = lambda out, items: copy_rows(out, [a for a, _ in items], [s[:1] for _, s in items])
        out = put(out, far2[2:] + [got0] + far3[:2])
        d_emb_table = put(out, [got1] + far3[2:])
        d_w_trans = gather_pieces([w_half, w_other], jnp.stack([plane, 1 - plane]).astype(I32)).reshape(width, width)
        vec = grads[hw:hw + 3]
        mlm_loss = grads[hw + 3, 0]
        d_b_vocab = jnp.concatenate([db_sh, jnp.where(core == 0, dl_mine, dl_other), jnp.where(core == 0, dl_other, dl_mine)])
        return mlm_loss, d_hidden, d_w_trans, vec[0], vec[1], vec[2], d_emb_table, d_b_vocab

    in_specs = (P("dp", None, None), P("dp", None), P("dp", None), P(None, None), P(None), P(None), P(None), P("vp", None), P("vp"))
    out_specs = (P(), P("dp", None, None), P(None, None), P(None), P(None), P(None), P("vp", None), P("vp"))

    return jax.shard_map(local_step, mesh=mesh, in_specs=in_specs, out_specs=out_specs, check_vma=False)
```

```python
import functools
import math

import jax
import jax.numpy as jnp
from jax import lax
from jax.experimental import pallas as pl
from jax.experimental.pallas import tpu as pltpu
from jax.sharding import PartitionSpec as P


LN_EPS = 1e-5

BF16, F32, I32 = jnp.bfloat16, jnp.float32, jnp.int32
SLOTS = 80
OWN_SPLIT = 7
VT = 2304
CHUNK = 768
SHARE_CHUNKS, SHARE_TILE = 4, 624
LOCAL_TILES, LOCAL_TILE = 6, 432
LOCAL_CALLS = 2
TOK_CHUNK = 1280
VMEM_ROWS = 44
COST_SCALE = 4
OFF = 1e30
SHORT = 10 ** 9
MIB, LANES, UNIT = 2 ** 20, 128, 16
SQRT_HALF, GAUSS = 0.5 ** 0.5, (2.0 * math.pi) ** -0.5


ANY_SPACE = pl.BlockSpec(memory_space=pl.ANY)


def fixed(shape):
    return pl.BlockSpec(shape, lambda *_: (0,) * len(shape))


def stepped(shape, base=0):
    return pl.BlockSpec(shape, lambda i, *_: (i + base,) + (0,) * (len(shape) - 1))


def row(x, k):
    return x[k:k + 1, :]


def lanes_of(x, k):
    return x[:, k * LANES:(k + 1) * LANES]


def fold(x):
    return functools.reduce(jnp.add, [lanes_of(x, k) for k in range(x.shape[1] // LANES)])


def wide(x, n):
    return jnp.concatenate([x] * (n // LANES), axis=1)


def row_sum(x):
    return jnp.sum(x, axis=1, keepdims=True)


def col_sum(x):
    return jnp.sum(x, axis=0, keepdims=True)


def row_mean(x):
    return jnp.mean(x, axis=1, keepdims=True)


def units(start, size):
    return pl.ds(pl.multiple_of(start * UNIT, UNIT), size)


def vmem_mib(n):
    return pltpu.CompilerParams(vmem_limit_bytes=n * MIB)


def cost(flops, bytes_accessed, transcendentals=0):
    return pl.CostEstimate(flops=flops, bytes_accessed=bytes_accessed, transcendentals=transcendentals)


def dot_nt(a, b):
    return lax.dot_general(a, b, (((1,), (1,)), ((), ())), preferred_element_type=F32)


def to_lanes(row):
    return jnp.broadcast_to(row, (128, row.shape[1])).T


def front_kernel(n_steps, hid_ref, pos_ref, w_ref, vec_ref, z_ref, pre_ref, u_ref, uf_ref):
    step = pl.program_id(0)
    pos = to_lanes(pos_ref[0])[:SLOTS]
    lane = lax.broadcasted_iota(I32, (SLOTS, 128), 1).astype(F32)
    hot = jnp.concatenate([jnp.where(pos == lane + k * 128.0, 1.0, 0.0) for k in range(hid_ref.shape[1] // 128)], axis=1)
    rows = pl.ds(pl.multiple_of(step * SLOTS, 16), SLOTS)
    z_ref[rows, :] = jnp.dot(hot.astype(BF16), hid_ref[0], preferred_element_type=F32).astype(BF16)

    @pl.when(step == n_steps - 1)
    def _():
        pre = jnp.dot(z_ref[...], w_ref[...], preferred_element_type=F32) + row(vec_ref, 0)
        pre_ref[...] = pre
        act = 0.5 * pre * (1.0 + lax.erf(pre * SQRT_HALF))
        cen = act - row_mean(act)
        var = row_mean(cen * cen)
        u = (cen * lax.rsqrt(var + LN_EPS) * row(vec_ref, 1) + row(vec_ref, 2)).astype(BF16)
        u_ref[...] = u
        uf_ref[...] = u.astype(F32)


def head_kernel(n_pieces, where_ref, pre_ref, mine_ref, other_ref, z_ref, w_ref, vec_ref, loss_ref, *refs):
    pieces, dz_ref, sum_ref = refs[:n_pieces], refs[n_pieces], refs[-1]
    pre = pre_ref[...]
    cdf = 0.5 * (1.0 + lax.erf(pre * SQRT_HALF))
    act = pre * cdf
    cen = act - row_mean(act)
    rstd = lax.rsqrt(row_mean(cen * cen) + LN_EPS)
    unit = cen * rstd
    du = mine_ref[...] + other_ref[...]
    dunit = du * row(vec_ref, 1)
    dact = rstd * (dunit - row_mean(dunit) - unit * row_mean(dunit * unit))
    dpre = dact * (cdf + pre * (jnp.exp(-0.5 * pre * pre) * GAUSS))
    dab = dpre.astype(BF16)
    dz_ref[...] = dot_nt(dab, w_ref[...]).astype(BF16)
    half = z_ref.shape[1] // 2
    z_half = z_ref[:, pl.ds(pl.multiple_of(where_ref[n_pieces] * half, 128), half)]
    sum_ref[...] = jnp.zeros_like(sum_ref)
    sum_ref[:half, :] = lax.dot_general(z_half, dab, (((0,), (0,)), ((), ())), preferred_element_type=F32)
    rows = [col_sum(dpre), col_sum(du * unit), col_sum(du), loss_ref[...]]
    for k, value in enumerate(rows):
        sum_ref[half + k:half + k + 1, :] = value
    size = sum_ref.shape[0] // n_pieces
    for k in range(n_pieces):
        pieces[k][...] = sum_ref[pl.ds(pl.multiple_of(where_ref[k] * size, 8), size), :]


def own_kernel(n_steps, first, u_ref, emb_ref, bias_ref, col_ref, lab_row_ref, *refs):
    acc_in, state_in = (None, None) if first else refs[:2]
    acc_ref, stat_ref, m_ref, s_ref, t_ref, lab_ref = refs if first else refs[2:]
    step = pl.program_id(0)

    @pl.when(step == 0)
    def _():
        lab_ref[...] = to_lanes(lab_row_ref[...])
        if first:
            m_ref[...] = jnp.full_like(m_ref, -1e38)
            s_ref[...] = jnp.zeros_like(s_ref)
            t_ref[...] = jnp.zeros_like(t_ref)
            acc_ref[...] = jnp.zeros_like(acc_ref)
        else:
            for k, ref in enumerate((m_ref, s_ref, t_ref)):
                ref[...] = state_in[k]
            acc_ref[...] = acc_in[...]

    logit = lambda q: dot_nt(u_ref[...], emb_ref[q * CHUNK:(q + 1) * CHUNK, :]) + bias_ref[0, :, q * CHUNK:(q + 1) * CHUNK]
    following = logit(0)
    for q in range(VT // CHUNK):
        block, cs = following, slice(q * CHUNK, (q + 1) * CHUNK)
        if q + 1 < VT // CHUNK:
            following = logit(q + 1)
        hot = col_ref[0, :, cs] == wide(lab_ref[...], CHUNK)
        m_old = m_ref[...]
        m_new = jnp.maximum(m_old, jnp.max(block, axis=1, keepdims=True))
        scale = jnp.exp(m_old - m_new)
        prob = jnp.exp(block - wide(m_new, CHUNK))
        m_ref[...] = m_new
        s_ref[...] = s_ref[...] * scale + fold(prob)
        t_ref[...] += fold(jnp.where(hot, block, 0.0))
        rest = jnp.where(hot, 0.0, prob).astype(BF16)
        acc_ref[...] = acc_ref[...] * wide(scale, acc_ref.shape[1]) + jnp.dot(rest, emb_ref[cs, :], preferred_element_type=F32)

    @pl.when(step == n_steps - 1)
    def _():
        if first:
            for k, ref in enumerate((m_ref, s_ref, t_ref)):
                stat_ref[k] = ref[...]
            return
        mass = row_sum(s_ref[...])
        target = row_sum(t_ref[...])
        lane = lax.broadcasted_iota(I32, m_ref.shape, 1)
        stat_ref[...] = jnp.where(lane == 0, m_ref[...], jnp.where(lane == 1, mass, target)).T[:8]


def norm_kernel(n_masks, inv_n, shard_rows, plane_ref, mine_ref, other_ref, lab_ref, tok_ref, coef_ref, loss_ref):
    low = plane_ref[0] == 0
    mine, other = mine_ref[...], other_ref[...]
    lo, hi = jnp.where(low, mine, other), jnp.where(low, other, mine)
    top = jnp.maximum(row(lo, 0), row(hi, 0))
    log_norm = top + jnp.log(row(lo, 1) * jnp.exp(row(lo, 0) - top) + row(hi, 1) * jnp.exp(row(hi, 0) - top))
    valid = lax.rem(lax.broadcasted_iota(I32, log_norm.shape, 1), SLOTS) < n_masks
    norm = jnp.where(valid, log_norm, OFF)
    lab = lab_ref[...]
    tok_ref[0:1, :] = norm
    tok_ref[1:2, :] = lab
    here = (lab >= 0.0) & (lab < shard_rows)
    coef_ref[0:1, :] = jnp.exp(row(mine, 0) - norm) * inv_n
    coef_ref[1:2, :] = jnp.where(here, (jnp.exp(row(mine, 2) - norm) - 1.0) * inv_n, 0.0)
    loss = jnp.sum(jnp.where(valid, log_norm - (row(lo, 2) + row(hi, 2)), 0.0), axis=1, keepdims=True) * inv_n
    loss_ref[...] = jnp.broadcast_to(loss, loss_ref.shape)


def du_kernel(acc_ref, row_ref, coef_ref, du_ref):
    width = acc_ref.shape[1]
    hot = to_lanes(row(coef_ref, 1)).astype(BF16).astype(F32)
    du = acc_ref[...] * wide(to_lanes(row(coef_ref, 0)), width) + row_ref[...].astype(F32) * wide(hot, width)
    du_ref[...] = du.astype(BF16).astype(F32)


def place_kernel(n, start_ref, *refs):
    pieces, out_ref, bufs, sems = refs[:n], refs[n], refs[n + 1:-1], refs[-1]
    loads = [pltpu.make_async_copy(pieces[k], bufs[k], sems.at[k]) for k in range(n)]
    for load in loads:
        load.start()
    for k in range(n):
        loads[k].wait()
        out_ref[units(start_ref[k], pieces[k].shape[0]), :] = bufs[k][...].astype(BF16)


def place(pieces, starts, n_all):
    n, width = len(pieces), pieces[0].shape[1]
    return pl.pallas_call(
        functools.partial(place_kernel, n),
        grid_spec=pltpu.PrefetchScalarGridSpec(
            num_scalar_prefetch=1,
            grid=(1,),
            in_specs=[ANY_SPACE] * n,
            out_specs=pl.BlockSpec(memory_space=pltpu.VMEM),
            scratch_shapes=[pltpu.VMEM(p.shape, F32) for p in pieces] + [pltpu.SemaphoreType.DMA((n,))],
        ),
        out_shape=jax.ShapeDtypeStruct((n_all, width), BF16),
        compiler_params=vmem_mib(40),
        cost_estimate=cost(SHORT, 6 * n_all * width),
    )(starts, *pieces)


def tok_kernel(n, start_ref, *refs):
    for k in range(n):
        place_at = pl.ds(start_ref[k], 1)
        refs[n][place_at, :] = row(refs[k], 0)
        refs[n + 1][place_at, :] = row(refs[k], 1)


def place_toks(toks, ranks):
    n, width = len(toks), toks[0].shape[1]
    return pl.pallas_call(
        functools.partial(tok_kernel, n),
        grid_spec=pltpu.PrefetchScalarGridSpec(
            num_scalar_prefetch=1,
            grid=(1,),
            in_specs=[fixed(t.shape) for t in toks],
            out_specs=[fixed((n, width))] * 2,
        ),
        out_shape=[jax.ShapeDtypeStruct((n, width), F32)] * 2,
    )(ranks, *toks)


def piece_kernel(n, start_ref, *refs):
    for k in range(n):
        refs[n][start_ref[k]] = refs[k][...]


def gather_pieces(pieces, ranks):
    n = len(pieces)
    shape = (n,) + pieces[0].shape
    return pl.pallas_call(
        functools.partial(piece_kernel, n),
        grid_spec=pltpu.PrefetchScalarGridSpec(
            num_scalar_prefetch=1,
            grid=(1,),
            in_specs=[fixed(p.shape) for p in pieces],
            out_specs=fixed(shape),
        ),
        out_shape=jax.ShapeDtypeStruct(shape, F32),
    )(ranks, *pieces)


def join_kernel(n, start_ref, *refs):
    head, rest, buf = refs[n:]
    size = refs[0].shape[0]
    for k in range(n):
        buf[pl.ds(pl.multiple_of(start_ref[k] * size, 8), size), :] = refs[k][...]
    cut = head.shape[0]
    head[...] = buf[:cut, :]
    rest[...] = buf[cut:, :]


def join_pieces(pieces, ranks, cut):
    n, (size, width) = len(pieces), pieces[0].shape
    shapes = [(cut, width), (n * size - cut, width)]
    return pl.pallas_call(
        functools.partial(join_kernel, n),
        grid_spec=pltpu.PrefetchScalarGridSpec(
            num_scalar_prefetch=1,
            grid=(1,),
            in_specs=[fixed(p.shape) for p in pieces],
            out_specs=[fixed(shape) for shape in shapes],
            scratch_shapes=[pltpu.VMEM((n * size, width), F32)],
        ),
        out_shape=[jax.ShapeDtypeStruct(shape, F32) for shape in shapes],
    )(ranks, *pieces)


def rows_kernel(cfg, start_ref, emb_ref, bias_ref, u_ref, norm_ref, lab_ref, *refs):
    n_steps, tile, inv_n, n_send, n_copy, aliased = cfg
    arrived, refs = refs[:n_copy], refs[n_copy + (1 if aliased else 0):]
    out_ref, db_ref, *refs = refs
    sends, refs = refs[:n_send], refs[n_send:]
    acc_ref, out_sem, send_sem = refs[:3]
    stage, (load_sem, store_sem) = (refs[3:-2], refs[-2:]) if n_copy else ((), (None, None))
    step = pl.program_id(0)
    slot = lax.rem(step, 2)
    n_tok = u_ref.shape[0]

    def load(k):
        return pltpu.make_async_copy(arrived[k], stage[k], load_sem.at[k])

    def store(k):
        rows = units(start_ref[2 * n_steps + k], arrived[k].shape[0])
        return pltpu.make_async_copy(stage[k], out_ref.at[rows, :], store_sem.at[k])

    @pl.when(step == 0)
    def _():
        for k in range(n_copy):
            load(k).start()

    @pl.when(step == 1)
    def _():
        for k in range(n_copy):
            load(k).wait()
            store(k).start()

    def out_copy(t, which):
        rows = units(start_ref[t], tile)
        return pltpu.make_async_copy(acc_ref.at[which], out_ref.at[rows, :], out_sem.at[which])

    def send_copy(t, which):
        rows = pl.ds(pl.multiple_of(t * tile, 16), tile) if n_send == 1 else pl.ds(0, tile)
        target = sends[0] if n_send == 1 else sends[t]
        return pltpu.make_async_copy(acc_ref.at[which], target.at[rows, :], send_sem.at[which])

    @pl.when(step >= 2)
    def _():
        out_copy(step - 2, slot).wait()
        pltpu.make_async_copy(acc_ref.at[slot], sends[0].at[pl.ds(0, tile), :], send_sem.at[slot]).wait()

    row_id = lax.broadcasted_iota(I32, (tile, 1), 0).astype(F32) + (start_ref[step] * 16).astype(F32)
    bias = wide(to_lanes(bias_ref[0])[:tile], TOK_CHUNK)
    per = TOK_CHUNK // norm_ref.shape[1]
    for j in range(n_tok // TOK_CHUNK):
        s = slice(j * TOK_CHUNK, (j + 1) * TOK_CHUNK)
        norm = jnp.concatenate([row(norm_ref, i) for i in range(j * per, (j + 1) * per)], axis=1)
        lab = jnp.concatenate([row(lab_ref, i) for i in range(j * per, (j + 1) * per)], axis=1)
        logit = dot_nt(emb_ref[...], u_ref[s, :]) + bias
        prob = jnp.exp(logit - norm)
        grad = (prob - jnp.where(lab == row_id, 1.0, 0.0)) * inv_n
        part = jnp.dot(grad.astype(BF16), u_ref[s, :], preferred_element_type=F32)
        db = fold(grad) if j == 0 else db + fold(grad)
        if j == 0:
            acc_ref[slot] = part
        else:
            acc_ref[slot] += part

    db = jnp.concatenate([db, jnp.zeros((db_ref.shape[2] - tile, 128), F32)])
    db_ref[0] = col_sum(db.T)
    out_copy(step, slot).start()
    if n_send == 1:
        send_copy(step, slot).start()
    else:
        for t in range(n_send):
            @pl.when(step == t)
            def _():
                send_copy(t, t % 2).start()

    @pl.when(step == n_steps - 1)
    def _():
        for k in range(n_copy):
            store(k).wait()
        for t in range(max(0, n_steps - 2), n_steps):
            out_copy(t, t % 2).wait()
            pltpu.make_async_copy(acc_ref.at[t % 2], sends[0].at[pl.ds(0, tile), :], send_sem.at[t % 2]).wait()


def emb_rows(out, starts, blocks, emb, bias, u_all, norm, lab, inv_n, tile, n_steps, n_send, arrived, copy_starts):
    n_tok, width = u_all.shape
    n_rows = emb.shape[0]
    n_copy = len(arrived)
    aliased = out is not None
    cfg = (n_steps, tile, inv_n, n_send, n_copy, aliased)
    table = jnp.concatenate([starts, blocks] + list(copy_starts)).astype(I32)
    any_space = ANY_SPACE
    whole = lambda a: fixed(a.shape)
    send_rows = n_steps * tile if n_send == 1 else tile
    scratch = [pltpu.VMEM((2, tile, width), F32), pltpu.SemaphoreType.DMA((2,)), pltpu.SemaphoreType.DMA((2,))]
    if n_copy:
        scratch += [pltpu.VMEM(a.shape, F32) for a in arrived] + [pltpu.SemaphoreType.DMA((n_copy,))] * 2
    return pl.pallas_call(
        functools.partial(rows_kernel, cfg),
        grid_spec=pltpu.PrefetchScalarGridSpec(
            num_scalar_prefetch=1,
            grid=(n_steps,),
            in_specs=[
                pl.BlockSpec((pl.Element(tile), pl.Element(width)), lambda i, s: (pl.multiple_of(s[i] * 16, 16), 0)),
                pl.BlockSpec((1, 1, bias.shape[2]), lambda i, s: (s[n_steps + i], 0, 0)),
                pl.BlockSpec(memory_space=pltpu.VMEM), whole(norm), whole(lab),
            ] + [any_space] * (n_copy + aliased),
            out_specs=[any_space, stepped((1, 1, bias.shape[2]))] + [any_space] * n_send,
            scratch_shapes=scratch,
        ),
        out_shape=[jax.ShapeDtypeStruct((n_rows, width), F32), jax.ShapeDtypeStruct((n_steps, 1, bias.shape[2]), F32)] + [jax.ShapeDtypeStruct((send_rows, width), F32)] * n_send,
        input_output_aliases={6 + n_copy: 0} if aliased else {},
        compiler_params=vmem_mib(VMEM_ROWS),
        cost_estimate=pl.CostEstimate(
            flops=n_steps * tile * n_tok * width // COST_SCALE, bytes_accessed=n_steps * tile * width * 10, transcendentals=n_steps * tile * n_tok
        ),
    )(table, emb, bias, u_all, norm, lab, *arrived, *([out] if aliased else []))


def copy_kernel(n, start_ref, *refs):
    arrived, (_, out_ref, *stage, load_sem, store_sem) = refs[:n], refs[n:]
    loads = [pltpu.make_async_copy(arrived[k], stage[k], load_sem.at[k]) for k in range(n)]
    for load in loads:
        load.start()
    stores = []
    for k in range(n):
        loads[k].wait()
        rows = units(start_ref[k], arrived[k].shape[0])
        stores.append(pltpu.make_async_copy(stage[k], out_ref.at[rows, :], store_sem.at[k]))
        stores[-1].start()
    for store in stores:
        store.wait()


def copy_rows(out, arrived, starts):
    n = len(arrived)
    return pl.pallas_call(
        functools.partial(copy_kernel, n),
        grid_spec=pltpu.PrefetchScalarGridSpec(
            num_scalar_prefetch=1,
            grid=(1,),
            in_specs=[ANY_SPACE] * (n + 1),
            out_specs=ANY_SPACE,
            scratch_shapes=[pltpu.VMEM(a.shape, F32) for a in arrived] + [pltpu.SemaphoreType.DMA((n,))] * 2,
        ),
        out_shape=jax.ShapeDtypeStruct(out.shape, F32),
        input_output_aliases={n + 1: 0},
        compiler_params=vmem_mib(48),
        cost_estimate=cost(SHORT, 8 * sum(a.size for a in arrived)),
    )(jnp.concatenate(starts).astype(I32), *arrived, out)


def swap(x, mask, axis="dp"):
    n = 8 if axis == "dp" else 2
    return lax.ppermute(x, axis, [(i, i ^ mask) for i in range(n)])


def solution(mesh):
    n_groups = mesh.shape["dp"]

    def local_step(hidden, mask_pos, labels, w_trans, b_trans, ln_gain, ln_bias, emb_table, b_vocab):
        n_rows, seq_len, width = hidden.shape
        n_masks = mask_pos.shape[1]
        shard_rows = emb_table.shape[0]
        inv_n = 1.0 / (n_rows * n_masks * n_groups)
        n_own = n_rows * SLOTS
        n_all = n_own * n_groups
        me, plane = lax.axis_index("dp"), lax.axis_index("vp")
        core, par = me & 1, ((me >> 1) ^ (me >> 2)) & 1
        row_start = plane * shard_rows

        pos = jnp.pad(mask_pos, ((0, 0), (0, SLOTS - n_masks)), constant_values=-1)
        pos_onehot = (pos[:, :, None] == jnp.arange(seq_len)[None, None, :]).astype(BF16)
        pos_row = jnp.pad(mask_pos, ((0, 0), (0, 128 - n_masks)), constant_values=-1).astype(F32)[:, None, :]
        tok_f32, tok_bf16 = jax.ShapeDtypeStruct((n_own, width), F32), jax.ShapeDtypeStruct((n_own, width), BF16)
        own_block = fixed((n_own, width))
        vectors = jnp.stack([b_trans, ln_gain, ln_bias])
        masked_h, pre_act, u_own, u_f = pl.pallas_call(
            functools.partial(front_kernel, n_rows),
            grid=(n_rows,),
            in_specs=[
                stepped((1, seq_len, width)), stepped((1, 1, 128)),
                fixed((width, width)), fixed((3, width)),
            ],
            out_specs=[own_block] * 4,
            out_shape=[tok_bf16, tok_f32, tok_bf16, tok_f32],
            compiler_params=vmem_mib(48),
            cost_estimate=cost(2 * n_own * width * (width + seq_len), 2 * hidden.size),
        )(hidden, pos_row, w_trans, vectors)

        half = n_own // 2
        u_sib, u_x, u_y = swap(u_f, 1), swap(u_f, 2), swap(u_f, 4)
        blk = n_own // 16

        n_steps = -(-shard_rows // VT)
        last = shard_rows - VT
        dup = n_steps * VT - shard_rows
        b_pad = jnp.concatenate([b_vocab[:shard_rows - (VT - dup)], jnp.full((dup,), -OFF, F32), b_vocab[shard_rows - (VT - dup):]]).reshape(n_steps, 1, VT)
        ids = jnp.arange(shard_rows, dtype=F32)
        cols = jnp.concatenate([ids[:shard_rows - (VT - dup)], jnp.full((dup,), -7.0, F32), ids[shard_rows - (VT - dup):]]).reshape(n_steps, 1, VT)
        lab_pad = jnp.pad(labels, ((0, 0), (0, SLOTS - n_masks)), constant_values=-1000000).reshape(n_own)
        lab_rel = (lab_pad - row_start).astype(F32)
        lab_row = lab_rel[None]
        row_block = fixed((1, n_own))
        state = jax.ShapeDtypeStruct((3, n_own, 128), F32)
        state_block = fixed(state.shape)

        def own_call(begin, end, carry):
            first = not carry
            skip = lambda i: i + begin
            last_shape = state if first else jax.ShapeDtypeStruct((8, n_own), F32)
            return pl.pallas_call(
                functools.partial(own_kernel, end - begin, first),
                grid=(end - begin,),
                in_specs=[
                    own_block,
                    pl.BlockSpec((pl.Element(VT), pl.Element(width)), lambda i: (pl.multiple_of(jnp.minimum(skip(i) * (VT // 16), last // 16) * 16, 16), 0)),
                    stepped((1, 1, VT), begin), stepped((1, 1, VT), begin), row_block,
                ] + ([] if first else [own_block, state_block]),
                out_specs=[own_block, state_block if first else fixed((8, n_own))],
                out_shape=[tok_f32, last_shape],
                scratch_shapes=[pltpu.VMEM((n_own, 128), F32)] * 4,
                compiler_params=vmem_mib(56),
                cost_estimate=pl.CostEstimate(
                    flops=4 * n_own * (end - begin) * VT * width // COST_SCALE, bytes_accessed=2 * (end - begin) * VT * width, transcendentals=n_own * shard_rows),
            )(u_own, emb_table, b_pad, cols, lab_row, *carry)

        carry = own_call(0, OWN_SPLIT, ())
        u_x, u_y, carry = lax.optimization_barrier((u_x, u_y, carry))
        u_d0, u_d1 = swap(u_x[:half], 4), swap(u_y[half:], 2)
        u_xs, u_ys = swap(u_x, 1), swap(u_y, 1)
        du_sum, stats = own_call(OWN_SPLIT, n_steps, carry)
        lab_local = lab_pad - row_start
        spread = jnp.arange(n_own, dtype=I32) * (shard_rows // n_own)
        label_rows = jnp.take(emb_table, jnp.where((lab_local >= 0) & (lab_local < shard_rows), lab_local, spread), axis=0)
        other = swap(stats, 1, "vp")
        (u_d0, u_d1), du_sum = lax.optimization_barrier(((u_d0, u_d1), du_sum))
        u_ds0, u_ds1 = swap(u_d0, 1), swap(u_d1, 1)

        ranks = jnp.stack([me ^ m for m in range(n_groups)]).astype(I32)
        split = jnp.repeat(ranks[6:], 2) * blk + jnp.tile(jnp.array([0, blk // 2], I32), 2)
        u_starts = jnp.concatenate([ranks[:6] * blk, split])
        u_all = place(
            [u_f, u_sib, u_x, u_xs, u_y, u_ys, u_d0, u_d1, u_ds0, u_ds1],
            u_starts, n_all)
        tok, coef, loss_row = pl.pallas_call(
            functools.partial(norm_kernel, n_masks, inv_n, shard_rows),
            in_specs=[pl.BlockSpec(memory_space=pltpu.SMEM)] + [pl.BlockSpec(memory_space=pltpu.VMEM)] * 3,
            out_shape=[jax.ShapeDtypeStruct((2, n_own), F32)] * 2 + [jax.ShapeDtypeStruct((1, width), F32)],
        )(plane[None], stats, other, lab_row)
        toks = [tok] + [swap(tok, m) for m in range(1, n_groups)]
        du_part = pl.pallas_call(
            du_kernel, out_shape=tok_f32, compiler_params=vmem_mib(32),
            cost_estimate=cost(SHORT, 10 * n_own * width),
        )(du_sum, label_rows, coef)
        du_other = swap(du_part, 1, "vp")
        norm_all, lab_all = place_toks(toks, ranks)

        nx, nl = SHARE_CHUNKS * SHARE_TILE // 16, LOCAL_TILES * LOCAL_TILE // 16
        assert 16 * (8 * nx + 2 * nl) == shard_rows
        st = SHARE_TILE // 16
        x_at = lambda p, c, k: ((2 * p + c) * nx + k * st)[None]
        y_at = lambda p, c, k: (4 * nx + (2 * p + c) * nx + k * st)[None]
        pad128 = lambda x: jnp.pad(x, ((0, 0), (0, -x.shape[1] % 128)))[:, None, :]
        bias_share = pad128(b_vocab[:16 * 8 * nx].reshape(-1, SHARE_TILE))
        bias_local = pad128(b_vocab[16 * 8 * nx:].reshape(-1, LOCAL_TILE))
        lt = LOCAL_TILE // 16
        out = None

        def rows_call(out, starts, blocks, bias, tile, n_steps, n_send, take):
            return emb_rows(out, starts, blocks, emb_table, bias, u_all, norm_all, lab_all, inv_n, tile, n_steps, n_send,
                            [a for a, _ in take], [s[:1] for _, s in take])

        per = LOCAL_TILES // LOCAL_CALLS
        l_at = lambda c, k: jnp.stack([8 * nx + c * nl + (k * per + i) * lt for i in range(per)])

        def shared_rows(out, k, take):
            starts = jnp.concatenate([x_at(par, core, k), y_at(par, core, k)])
            return rows_call(out, starts, starts // st, bias_share, SHARE_TILE, 2, 2, take)

        def local_rows(out, k, take):
            starts = l_at(core, k)
            out, db, rows = rows_call(out, starts, (starts - 8 * nx) // lt, bias_local, LOCAL_TILE, per, 1, take)
            return out, (swap(rows, 1), l_at(1 - core, k)), db[:, 0, :LOCAL_TILE]

        def near(k, sx, sy):
            return [(swap(sx, 1), x_at(par, 1 - core, k)), (swap(sy, 1), y_at(par, 1 - core, k))]

        def far(k, rx, ry):
            return [(rx, x_at(1 - par, core, k)), (ry, y_at(1 - par, core, k)),
                    (swap(rx, 1), x_at(1 - par, 1 - core, k)),
                    (swap(ry, 1), y_at(1 - par, 1 - core, k))]

        after = lax.optimization_barrier
        out, db0, sx0, sy0 = shared_rows(out, 0, [])
        rx0, ry0 = swap(sx0, 2), swap(sy0, 4)
        near0 = near(0, sx0, sy0)
        out, db1, sx1, sy1 = shared_rows(out, 1, [])
        rx1, ry1 = swap(sx1, 2), swap(sy1, 4)
        near1 = near(1, sx1, sy1)

        du_other, out = after((du_other, out))
        hw = width // 2
        padded = -(-(hw + 4) // 64) * 64
        part = jax.ShapeDtypeStruct((padded // n_groups, width), F32)
        vmem = pl.BlockSpec(memory_space=pltpu.VMEM)
        *parts, d_masked = pl.pallas_call(
            functools.partial(head_kernel, n_groups),
            in_specs=[pl.BlockSpec(memory_space=pltpu.SMEM)] + [vmem] * 7,
            out_shape=[part] * n_groups + [tok_bf16],
            scratch_shapes=[pltpu.VMEM((padded, width), F32)],
            compiler_params=vmem_mib(40),
            cost_estimate=pl.CostEstimate(flops=3 * n_own * width * width, bytes_accessed=20 * n_own * width, transcendentals=2 * n_own * width),
        )(jnp.concatenate([ranks, plane[None]]), pre_act, du_part, du_other, masked_h, w_trans, vectors, loss_row)
        parts, out, d_masked = after((parts, out, d_masked))
        got = [swap(parts[m], m) for m in range(1, n_groups)]

        out, db2, sx2, sy2 = shared_rows(out, 2, [])
        near2 = near(2, sx2, sy2)
        out, rx0, ry0, sx2, sy2 = after((out, rx0, ry0, sx2, sy2))
        rx2, ry2 = swap(sx2, 2), swap(sy2, 4)
        far0 = far(0, rx0, ry0)
        out, db3, sx3, sy3 = shared_rows(out, 3, near0 + near1)
        near3 = near(3, sx3, sy3)
        out, rx1, ry1, sx3, sy3, got = after((out, rx1, ry1, sx3, sy3, got))
        rx3, ry3 = swap(sx3, 2), swap(sy3, 4)
        far1 = far(1, rx1, ry1)
        parts = parts[:1] + got
        level = lambda v: [v[i] + v[i + 1] for i in range(0, len(v), 2)]
        acc = level(level(level(parts)))[0]
        db_mine = jnp.stack([jnp.concatenate([d[i, 0, :SHARE_TILE] for d in (db0, db1, db2, db3)]) for i in range(2)])
        acc, db_mine, out = after((acc, db_mine, out))
        sums = [acc] + [swap(acc, m) for m in range(1, n_groups)]
        db_rel = [db_mine] + [swap(db_mine, m) for m in (1, 2, 3)]
        out, got0, dl0 = local_rows(out, 0, near2 + far0)
        sums, out = after((sums, out))
        w_half, small = join_pieces(sums, ranks, hw)
        w_half, out = after((w_half, out))
        w_other = swap(w_half, 1, "vp")
        out, rx2, ry2, d_masked, db_rel = after((out, rx2, ry2, d_masked, db_rel))
        far2 = far(2, rx2, ry2)
        db_sh = jnp.stack(db_rel, 1).reshape(2, 2, 2, 16 * nx)
        db_sh = jnp.where(par == 1, jnp.flip(db_sh, 1), db_sh)
        db_sh = jnp.where(core == 1, jnp.flip(db_sh, 2), db_sh).reshape(2 * 4 * 16 * nx)
        out, got1, dl1 = local_rows(out, 1, near3 + far1 + far2[:2] + [got0])
        out, rx3, ry3 = after((out, rx3, ry3))
        far3 = far(3, rx3, ry3)
        dl_mine = jnp.concatenate([dl0, dl1]).reshape(16 * nl)
        dl_other = swap(dl_mine, 1)
        d_hidden = jnp.einsum("clt,cle->cte", pos_onehot, d_masked.reshape(n_rows, SLOTS, width), preferred_element_type=F32).astype(BF16)
        put = lambda out, items: copy_rows(out, [a for a, _ in items], [s[:1] for _, s in items])
        out = put(out, far2[2:] + far3[:2])
        d_emb_table = put(out, [got1] + far3[2:])
        d_w_trans = gather_pieces([w_half, w_other], jnp.stack([plane, 1 - plane]).astype(I32)).reshape(width, width)
        mlm_loss = small[3, 0]
        d_b_vocab = jnp.concatenate([db_sh, jnp.where(core == 0, dl_mine, dl_other), jnp.where(core == 0, dl_other, dl_mine)])
        return mlm_loss, d_hidden, d_w_trans, small[0], small[1], small[2], d_emb_table, d_b_vocab

    in_specs = (P("dp"), P("dp"), P("dp"), P(), P(), P(), P(), P("vp"), P("vp"))
    out_specs = (P(), P("dp"), P(), P(), P(), P(), P("vp"), P("vp"))

    return jax.shard_map(local_step, mesh=mesh, in_specs=in_specs, out_specs=out_specs, check_vma=False)
```

```python
import functools
import math

import jax
import jax.numpy as jnp
from jax import lax
from jax.experimental import pallas as pl
from jax.experimental.pallas import tpu as pltpu
from jax.sharding import PartitionSpec as P


LN_EPS = 1e-5

BF16, F32, I32 = jnp.bfloat16, jnp.float32, jnp.int32
SLOTS = 80
OWN_SPLIT = 7
VT = 2304
CHUNK = 768
SHARE_CHUNKS, SHARE_TILE = 4, 624
LOCAL_TILES, LOCAL_TILE = 6, 432
LOCAL_CALLS = 2
TOK_CHUNK = 1280
VMEM_ROWS = 44
COST_SCALE = 4
OFF = 1e30
SHORT = 10 ** 9
MIB, LANES, UNIT = 2 ** 20, 128, 16
SQRT_HALF, GAUSS = 0.5 ** 0.5, (2.0 * math.pi) ** -0.5


ANY_SPACE = pl.BlockSpec(memory_space=pl.ANY)


def fixed(shape):
    return pl.BlockSpec(shape, lambda *_: (0,) * len(shape))


def stepped(shape, base=0):
    return pl.BlockSpec(shape, lambda i, *_: (i + base,) + (0,) * (len(shape) - 1))


def row(x, k):
    return x[k:k + 1, :]


def lanes_of(x, k):
    return x[:, k * LANES:(k + 1) * LANES]


def fold(x):
    return functools.reduce(jnp.add, [lanes_of(x, k) for k in range(x.shape[1] // LANES)])


def wide(x, n):
    return jnp.concatenate([x] * (n // LANES), axis=1)


def row_sum(x):
    return jnp.sum(x, axis=1, keepdims=True)


def col_sum(x):
    return jnp.sum(x, axis=0, keepdims=True)


def row_mean(x):
    return jnp.mean(x, axis=1, keepdims=True)


def units(start, size):
    return pl.ds(pl.multiple_of(start * UNIT, UNIT), size)


def vmem_mib(n):
    return pltpu.CompilerParams(vmem_limit_bytes=n * MIB)


def cost(flops, bytes_accessed, transcendentals=0):
    return pl.CostEstimate(flops=flops, bytes_accessed=bytes_accessed, transcendentals=transcendentals)


def dot_nt(a, b):
    return lax.dot_general(a, b, (((1,), (1,)), ((), ())), preferred_element_type=F32)


def to_lanes(row):
    return jnp.broadcast_to(row, (128, row.shape[1])).T


def front_kernel(n_steps, hid_ref, pos_ref, w_ref, vec_ref, z_ref, pre_ref, u_ref, uf_ref):
    step = pl.program_id(0)
    pos = to_lanes(pos_ref[0])[:SLOTS]
    lane = lax.broadcasted_iota(I32, (SLOTS, 128), 1).astype(F32)
    hot = jnp.concatenate([jnp.where(pos == lane + k * 128.0, 1.0, 0.0) for k in range(hid_ref.shape[1] // 128)], axis=1)
    rows = pl.ds(pl.multiple_of(step * SLOTS, 16), SLOTS)
    z_ref[rows, :] = jnp.dot(hot.astype(BF16), hid_ref[0], preferred_element_type=F32).astype(BF16)

    @pl.when(step == n_steps - 1)
    def _():
        pre = jnp.dot(z_ref[...], w_ref[...], preferred_element_type=F32) + row(vec_ref, 0)
        pre_ref[...] = pre
        act = 0.5 * pre * (1.0 + lax.erf(pre * SQRT_HALF))
        cen = act - row_mean(act)
        var = row_mean(cen * cen)
        u = (cen * lax.rsqrt(var + LN_EPS) * row(vec_ref, 1) + row(vec_ref, 2)).astype(BF16)
        u_ref[...] = u
        uf_ref[...] = u.astype(F32)


def head_kernel(n_pieces, where_ref, pre_ref, mine_ref, other_ref, z_ref, w_ref, vec_ref, loss_ref, *refs):
    pieces, dz_ref, sum_ref = refs[:n_pieces], refs[n_pieces], refs[-1]
    pre = pre_ref[...]
    cdf = 0.5 * (1.0 + lax.erf(pre * SQRT_HALF))
    act = pre * cdf
    cen = act - row_mean(act)
    rstd = lax.rsqrt(row_mean(cen * cen) + LN_EPS)
    unit = cen * rstd
    du = mine_ref[...] + other_ref[...]
    dunit = du * row(vec_ref, 1)
    dact = rstd * (dunit - row_mean(dunit) - unit * row_mean(dunit * unit))
    dpre = dact * (cdf + pre * (jnp.exp(-0.5 * pre * pre) * GAUSS))
    dab = dpre.astype(BF16)
    dz_ref[...] = dot_nt(dab, w_ref[...]).astype(BF16)
    half = z_ref.shape[1] // 2
    z_half = z_ref[:, pl.ds(pl.multiple_of(where_ref[n_pieces] * half, 128), half)]
    sum_ref[...] = jnp.zeros_like(sum_ref)
    sum_ref[:half, :] = lax.dot_general(z_half, dab, (((0,), (0,)), ((), ())), preferred_element_type=F32)
    rows = [col_sum(dpre), col_sum(du * unit), col_sum(du), loss_ref[...]]
    for k, value in enumerate(rows):
        sum_ref[half + k:half + k + 1, :] = value
    size = sum_ref.shape[0] // n_pieces
    for k in range(n_pieces):
        pieces[k][...] = sum_ref[pl.ds(pl.multiple_of(where_ref[k] * size, 8), size), :]


def own_kernel(n_steps, first, u_ref, emb_ref, bias_ref, col_ref, lab_row_ref, *refs):
    acc_in, state_in = (None, None) if first else refs[:2]
    acc_ref, stat_ref, m_ref, s_ref, t_ref, lab_ref = refs if first else refs[2:]
    step = pl.program_id(0)

    @pl.when(step == 0)
    def _():
        lab_ref[...] = to_lanes(lab_row_ref[...])
        if first:
            m_ref[...] = jnp.full_like(m_ref, -1e38)
            s_ref[...] = jnp.zeros_like(s_ref)
            t_ref[...] = jnp.zeros_like(t_ref)
            acc_ref[...] = jnp.zeros_like(acc_ref)
        else:
            for k, ref in enumerate((m_ref, s_ref, t_ref)):
                ref[...] = state_in[k]
            acc_ref[...] = acc_in[...]

    logit = lambda q: dot_nt(u_ref[...], emb_ref[q * CHUNK:(q + 1) * CHUNK, :]) + bias_ref[0, :, q * CHUNK:(q + 1) * CHUNK]
    following = logit(0)
    for q in range(VT // CHUNK):
        block, cs = following, slice(q * CHUNK, (q + 1) * CHUNK)
        if q + 1 < VT // CHUNK:
            following = logit(q + 1)
        hot = col_ref[0, :, cs] == wide(lab_ref[...], CHUNK)
        m_old = m_ref[...]
        m_new = jnp.maximum(m_old, jnp.max(block, axis=1, keepdims=True))
        scale = jnp.exp(m_old - m_new)
        prob = jnp.exp(block - wide(m_new, CHUNK))
        m_ref[...] = m_new
        s_ref[...] = s_ref[...] * scale + fold(prob)
        t_ref[...] += fold(jnp.where(hot, block, 0.0))
        rest = jnp.where(hot, 0.0, prob).astype(BF16)
        acc_ref[...] = acc_ref[...] * wide(scale, acc_ref.shape[1]) + jnp.dot(rest, emb_ref[cs, :], preferred_element_type=F32)

    @pl.when(step == n_steps - 1)
    def _():
        if first:
            for k, ref in enumerate((m_ref, s_ref, t_ref)):
                stat_ref[k] = ref[...]
            return
        mass = row_sum(s_ref[...])
        target = row_sum(t_ref[...])
        lane = lax.broadcasted_iota(I32, m_ref.shape, 1)
        stat_ref[...] = jnp.where(lane == 0, m_ref[...], jnp.where(lane == 1, mass, target)).T[:8]


def norm_kernel(n_masks, inv_n, shard_rows, plane_ref, mine_ref, other_ref, lab_ref, tok_ref, coef_ref, loss_ref):
    low = plane_ref[0] == 0
    mine, other = mine_ref[...], other_ref[...]
    lo, hi = jnp.where(low, mine, other), jnp.where(low, other, mine)
    top = jnp.maximum(row(lo, 0), row(hi, 0))
    log_norm = top + jnp.log(row(lo, 1) * jnp.exp(row(lo, 0) - top) + row(hi, 1) * jnp.exp(row(hi, 0) - top))
    valid = lax.rem(lax.broadcasted_iota(I32, log_norm.shape, 1), SLOTS) < n_masks
    norm = jnp.where(valid, log_norm, OFF)
    lab = lab_ref[...]
    tok_ref[0:1, :] = norm
    tok_ref[1:2, :] = lab
    here = (lab >= 0.0) & (lab < shard_rows)
    coef_ref[0:1, :] = jnp.exp(row(mine, 0) - norm) * inv_n
    coef_ref[1:2, :] = jnp.where(here, (jnp.exp(row(mine, 2) - norm) - 1.0) * inv_n, 0.0)
    loss = jnp.sum(jnp.where(valid, log_norm - (row(lo, 2) + row(hi, 2)), 0.0), axis=1, keepdims=True) * inv_n
    loss_ref[...] = jnp.broadcast_to(loss, loss_ref.shape)


def du_kernel(acc_ref, row_ref, coef_ref, du_ref):
    width = acc_ref.shape[1]
    hot = to_lanes(row(coef_ref, 1)).astype(BF16).astype(F32)
    du = acc_ref[...] * wide(to_lanes(row(coef_ref, 0)), width) + row_ref[...].astype(F32) * wide(hot, width)
    du_ref[...] = du.astype(BF16).astype(F32)


def place_kernel(n, start_ref, *refs):
    pieces, out_ref, bufs, sems = refs[:n], refs[n], refs[n + 1:-1], refs[-1]
    loads = [pltpu.make_async_copy(pieces[k], bufs[k], sems.at[k]) for k in range(n)]
    for load in loads:
        load.start()
    for k in range(n):
        loads[k].wait()
        out_ref[units(start_ref[k], pieces[k].shape[0]), :] = bufs[k][...].astype(BF16)


def place(pieces, starts, n_all):
    n, width = len(pieces), pieces[0].shape[1]
    return pl.pallas_call(
        functools.partial(place_kernel, n),
        grid_spec=pltpu.PrefetchScalarGridSpec(
            num_scalar_prefetch=1,
            grid=(1,),
            in_specs=[ANY_SPACE] * n,
            out_specs=pl.BlockSpec(memory_space=pltpu.VMEM),
            scratch_shapes=[pltpu.VMEM(p.shape, F32) for p in pieces] + [pltpu.SemaphoreType.DMA((n,))],
        ),
        out_shape=jax.ShapeDtypeStruct((n_all, width), BF16),
        compiler_params=vmem_mib(40),
        cost_estimate=cost(SHORT, 6 * n_all * width),
    )(starts, *pieces)


def tok_kernel(n, start_ref, *refs):
    for k in range(n):
        place_at = pl.ds(start_ref[k], 1)
        refs[n][place_at, :] = row(refs[k], 0)
        refs[n + 1][place_at, :] = row(refs[k], 1)


def place_toks(toks, ranks):
    n, width = len(toks), toks[0].shape[1]
    return pl.pallas_call(
        functools.partial(tok_kernel, n),
        grid_spec=pltpu.PrefetchScalarGridSpec(
            num_scalar_prefetch=1,
            grid=(1,),
            in_specs=[fixed(t.shape) for t in toks],
            out_specs=[fixed((n, width))] * 2,
        ),
        out_shape=[jax.ShapeDtypeStruct((n, width), F32)] * 2,
    )(ranks, *toks)


def piece_kernel(n, start_ref, *refs):
    for k in range(n):
        refs[n][start_ref[k]] = refs[k][...]


def gather_pieces(pieces, ranks):
    n = len(pieces)
    shape = (n,) + pieces[0].shape
    return pl.pallas_call(
        functools.partial(piece_kernel, n),
        grid_spec=pltpu.PrefetchScalarGridSpec(
            num_scalar_prefetch=1,
            grid=(1,),
            in_specs=[fixed(p.shape) for p in pieces],
            out_specs=fixed(shape),
        ),
        out_shape=jax.ShapeDtypeStruct(shape, F32),
    )(ranks, *pieces)


def join_kernel(n, start_ref, *refs):
    head, rest, buf = refs[n:]
    size = refs[0].shape[0]
    for k in range(n):
        buf[pl.ds(pl.multiple_of(start_ref[k] * size, 8), size), :] = refs[k][...]
    cut = head.shape[0]
    head[...] = buf[:cut, :]
    rest[...] = buf[cut:, :]


def join_pieces(pieces, ranks, cut):
    n, (size, width) = len(pieces), pieces[0].shape
    shapes = [(cut, width), (n * size - cut, width)]
    return pl.pallas_call(
        functools.partial(join_kernel, n),
        grid_spec=pltpu.PrefetchScalarGridSpec(
            num_scalar_prefetch=1,
            grid=(1,),
            in_specs=[fixed(p.shape) for p in pieces],
            out_specs=[fixed(shape) for shape in shapes],
            scratch_shapes=[pltpu.VMEM((n * size, width), F32)],
        ),
        out_shape=[jax.ShapeDtypeStruct(shape, F32) for shape in shapes],
    )(ranks, *pieces)


def rows_kernel(cfg, start_ref, emb_ref, bias_ref, u_ref, norm_ref, lab_ref, *refs):
    n_steps, tile, inv_n, n_send, n_copy, aliased = cfg
    arrived, refs = refs[:n_copy], refs[n_copy + (1 if aliased else 0):]
    out_ref, db_ref, *refs = refs
    sends, refs = refs[:n_send], refs[n_send:]
    acc_ref, out_sem, send_sem = refs[:3]
    stage, (load_sem, store_sem) = (refs[3:-2], refs[-2:]) if n_copy else ((), (None, None))
    step = pl.program_id(0)
    slot = lax.rem(step, 2)
    n_tok = u_ref.shape[0]

    def load(k):
        return pltpu.make_async_copy(arrived[k], stage[k], load_sem.at[k])

    def store(k):
        rows = units(start_ref[2 * n_steps + k], arrived[k].shape[0])
        return pltpu.make_async_copy(stage[k], out_ref.at[rows, :], store_sem.at[k])

    @pl.when(step == 0)
    def _():
        for k in range(n_copy):
            load(k).start()

    @pl.when(step == 1)
    def _():
        for k in range(n_copy):
            load(k).wait()
            store(k).start()

    def out_copy(t, which):
        rows = units(start_ref[t], tile)
        return pltpu.make_async_copy(acc_ref.at[which], out_ref.at[rows, :], out_sem.at[which])

    def send_copy(t, which):
        rows = pl.ds(pl.multiple_of(t * tile, 16), tile) if n_send == 1 else pl.ds(0, tile)
        target = sends[0] if n_send == 1 else sends[t]
        return pltpu.make_async_copy(acc_ref.at[which], target.at[rows, :], send_sem.at[which])

    @pl.when(step >= 2)
    def _():
        out_copy(step - 2, slot).wait()
        pltpu.make_async_copy(acc_ref.at[slot], sends[0].at[pl.ds(0, tile), :], send_sem.at[slot]).wait()

    row_id = lax.broadcasted_iota(I32, (tile, 1), 0).astype(F32) + (start_ref[step] * 16).astype(F32)
    bias = wide(to_lanes(bias_ref[0])[:tile], TOK_CHUNK)
    per = TOK_CHUNK // norm_ref.shape[1]
    for j in range(n_tok // TOK_CHUNK):
        s = slice(j * TOK_CHUNK, (j + 1) * TOK_CHUNK)
        norm = jnp.concatenate([row(norm_ref, i) for i in range(j * per, (j + 1) * per)], axis=1)
        lab = jnp.concatenate([row(lab_ref, i) for i in range(j * per, (j + 1) * per)], axis=1)
        logit = dot_nt(emb_ref[...], u_ref[s, :]) + bias
        prob = jnp.exp(logit - norm)
        grad = (prob - jnp.where(lab == row_id, 1.0, 0.0)) * inv_n
        part = jnp.dot(grad.astype(BF16), u_ref[s, :], preferred_element_type=F32)
        db = fold(grad) if j == 0 else db + fold(grad)
        if j == 0:
            acc_ref[slot] = part
        else:
            acc_ref[slot] += part

    db = jnp.concatenate([db, jnp.zeros((db_ref.shape[2] - tile, 128), F32)])
    db_ref[0] = col_sum(db.T)
    out_copy(step, slot).start()
    if n_send == 1:
        send_copy(step, slot).start()
    else:
        for t in range(n_send):
            @pl.when(step == t)
            def _():
                send_copy(t, t % 2).start()

    @pl.when(step == n_steps - 1)
    def _():
        for k in range(n_copy):
            store(k).wait()
        for t in range(max(0, n_steps - 2), n_steps):
            out_copy(t, t % 2).wait()
            pltpu.make_async_copy(acc_ref.at[t % 2], sends[0].at[pl.ds(0, tile), :], send_sem.at[t % 2]).wait()


def emb_rows(out, starts, blocks, emb, bias, u_all, norm, lab, inv_n, tile, n_steps, n_send, arrived, copy_starts):
    n_tok, width = u_all.shape
    n_rows = emb.shape[0]
    n_copy = len(arrived)
    aliased = out is not None
    cfg = (n_steps, tile, inv_n, n_send, n_copy, aliased)
    table = jnp.concatenate([starts, blocks] + list(copy_starts)).astype(I32)
    any_space = ANY_SPACE
    whole = lambda a: fixed(a.shape)
    send_rows = n_steps * tile if n_send == 1 else tile
    scratch = [pltpu.VMEM((2, tile, width), F32), pltpu.SemaphoreType.DMA((2,)), pltpu.SemaphoreType.DMA((2,))]
    if n_copy:
        scratch += [pltpu.VMEM(a.shape, F32) for a in arrived] + [pltpu.SemaphoreType.DMA((n_copy,))] * 2
    return pl.pallas_call(
        functools.partial(rows_kernel, cfg),
        grid_spec=pltpu.PrefetchScalarGridSpec(
            num_scalar_prefetch=1,
            grid=(n_steps,),
            in_specs=[
                pl.BlockSpec((pl.Element(tile), pl.Element(width)), lambda i, s: (pl.multiple_of(s[i] * 16, 16), 0)),
                pl.BlockSpec((1, 1, bias.shape[2]), lambda i, s: (s[n_steps + i], 0, 0)),
                pl.BlockSpec(memory_space=pltpu.VMEM), whole(norm), whole(lab),
            ] + [any_space] * (n_copy + aliased),
            out_specs=[any_space, stepped((1, 1, bias.shape[2]))] + [any_space] * n_send,
            scratch_shapes=scratch,
        ),
        out_shape=[jax.ShapeDtypeStruct((n_rows, width), F32), jax.ShapeDtypeStruct((n_steps, 1, bias.shape[2]), F32)] + [jax.ShapeDtypeStruct((send_rows, width), F32)] * n_send,
        input_output_aliases={6 + n_copy: 0} if aliased else {},
        compiler_params=vmem_mib(VMEM_ROWS),
        cost_estimate=pl.CostEstimate(
            flops=n_steps * tile * n_tok * width // COST_SCALE, bytes_accessed=n_steps * tile * width * 10, transcendentals=n_steps * tile * n_tok
        ),
    )(table, emb, bias, u_all, norm, lab, *arrived, *([out] if aliased else []))


def copy_kernel(n, start_ref, *refs):
    arrived, (_, out_ref, *stage, load_sem, store_sem) = refs[:n], refs[n:]
    loads = [pltpu.make_async_copy(arrived[k], stage[k], load_sem.at[k]) for k in range(n)]
    for load in loads:
        load.start()
    stores = []
    for k in range(n):
        loads[k].wait()
        rows = units(start_ref[k], arrived[k].shape[0])
        stores.append(pltpu.make_async_copy(stage[k], out_ref.at[rows, :], store_sem.at[k]))
        stores[-1].start()
    for store in stores:
        store.wait()


def copy_rows(out, arrived, starts):
    n = len(arrived)
    return pl.pallas_call(
        functools.partial(copy_kernel, n),
        grid_spec=pltpu.PrefetchScalarGridSpec(
            num_scalar_prefetch=1,
            grid=(1,),
            in_specs=[ANY_SPACE] * (n + 1),
            out_specs=ANY_SPACE,
            scratch_shapes=[pltpu.VMEM(a.shape, F32) for a in arrived] + [pltpu.SemaphoreType.DMA((n,))] * 2,
        ),
        out_shape=jax.ShapeDtypeStruct(out.shape, F32),
        input_output_aliases={n + 1: 0},
        compiler_params=vmem_mib(48),
        cost_estimate=cost(SHORT, 8 * sum(a.size for a in arrived)),
    )(jnp.concatenate(starts).astype(I32), *arrived, out)


def swap(x, mask, axis="dp"):
    n = 8 if axis == "dp" else 2
    return lax.ppermute(x, axis, [(i, i ^ mask) for i in range(n)])


def solution(mesh):
    n_groups = mesh.shape["dp"]

    def local_step(hidden, mask_pos, labels, w_trans, b_trans, ln_gain, ln_bias, emb_table, b_vocab):
        n_rows, seq_len, width = hidden.shape
        n_masks = mask_pos.shape[1]
        shard_rows = emb_table.shape[0]
        inv_n = 1.0 / (n_rows * n_masks * n_groups)
        n_own = n_rows * SLOTS
        n_all = n_own * n_groups
        me, plane = lax.axis_index("dp"), lax.axis_index("vp")
        core, par = me & 1, ((me >> 1) ^ (me >> 2)) & 1
        row_start = plane * shard_rows

        pos = jnp.pad(mask_pos, ((0, 0), (0, SLOTS - n_masks)), constant_values=-1)
        pos_onehot = (pos[:, :, None] == jnp.arange(seq_len)[None, None, :]).astype(BF16)
        pos_row = jnp.pad(mask_pos, ((0, 0), (0, 128 - n_masks)), constant_values=-1).astype(F32)[:, None, :]
        tok_f32, tok_bf16 = jax.ShapeDtypeStruct((n_own, width), F32), jax.ShapeDtypeStruct((n_own, width), BF16)
        own_block = fixed((n_own, width))
        vectors = jnp.stack([b_trans, ln_gain, ln_bias])
        masked_h, pre_act, u_own, u_f = pl.pallas_call(
            functools.partial(front_kernel, n_rows),
            grid=(n_rows,),
            in_specs=[
                stepped((1, seq_len, width)), stepped((1, 1, 128)),
                fixed((width, width)), fixed((3, width)),
            ],
            out_specs=[own_block] * 4,
            out_shape=[tok_bf16, tok_f32, tok_bf16, tok_f32],
            compiler_params=vmem_mib(48),
            cost_estimate=cost(2 * n_own * width * (width + seq_len), 2 * hidden.size),
        )(hidden, pos_row, w_trans, vectors)

        half = n_own // 2
        u_sib, u_x, u_y = swap(u_f, 1), swap(u_f, 2), swap(u_f, 4)
        blk = n_own // 16

        n_steps = -(-shard_rows // VT)
        last = shard_rows - VT
        dup = n_steps * VT - shard_rows
        b_pad = jnp.concatenate([b_vocab[:shard_rows - (VT - dup)], jnp.full((dup,), -OFF, F32), b_vocab[shard_rows - (VT - dup):]]).reshape(n_steps, 1, VT)
        ids = jnp.arange(shard_rows, dtype=F32)
        cols = jnp.concatenate([ids[:shard_rows - (VT - dup)], jnp.full((dup,), -7.0, F32), ids[shard_rows - (VT - dup):]]).reshape(n_steps, 1, VT)
        lab_pad = jnp.pad(labels, ((0, 0), (0, SLOTS - n_masks)), constant_values=-1000000).reshape(n_own)
        lab_rel = (lab_pad - row_start).astype(F32)
        lab_row = lab_rel[None]
        row_block = fixed((1, n_own))
        state = jax.ShapeDtypeStruct((3, n_own, 128), F32)
        state_block = fixed(state.shape)

        def own_call(begin, end, carry):
            first = not carry
            skip = lambda i: i + begin
            last_shape = state if first else jax.ShapeDtypeStruct((8, n_own), F32)
            return pl.pallas_call(
                functools.partial(own_kernel, end - begin, first),
                grid=(end - begin,),
                in_specs=[
                    own_block,
                    pl.BlockSpec((pl.Element(VT), pl.Element(width)), lambda i: (pl.multiple_of(jnp.minimum(skip(i) * (VT // 16), last // 16) * 16, 16), 0)),
                    stepped((1, 1, VT), begin), stepped((1, 1, VT), begin), row_block,
                ] + ([] if first else [own_block, state_block]),
                out_specs=[own_block, state_block if first else fixed((8, n_own))],
                out_shape=[tok_f32, last_shape],
                scratch_shapes=[pltpu.VMEM((n_own, 128), F32)] * 4,
                compiler_params=vmem_mib(56),
                cost_estimate=pl.CostEstimate(
                    flops=4 * n_own * (end - begin) * VT * width // COST_SCALE, bytes_accessed=2 * (end - begin) * VT * width, transcendentals=n_own * shard_rows),
            )(u_own, emb_table, b_pad, cols, lab_row, *carry)

        carry = own_call(0, OWN_SPLIT, ())
        u_x, u_y, carry = lax.optimization_barrier((u_x, u_y, carry))
        u_d0, u_d1 = swap(u_x[:half], 4), swap(u_y[half:], 2)
        u_xs, u_ys = swap(u_x, 1), swap(u_y, 1)
        du_sum, stats = own_call(OWN_SPLIT, n_steps, carry)
        lab_local = lab_pad - row_start
        spread = jnp.arange(n_own, dtype=I32) * (shard_rows // n_own)
        label_rows = jnp.take(emb_table, jnp.where((lab_local >= 0) & (lab_local < shard_rows), lab_local, spread), axis=0)
        other = swap(stats, 1, "vp")
        (u_d0, u_d1), du_sum = lax.optimization_barrier(((u_d0, u_d1), du_sum))
        u_ds0, u_ds1 = swap(u_d0, 1), swap(u_d1, 1)

        ranks = jnp.stack([me ^ m for m in range(n_groups)]).astype(I32)
        split = jnp.repeat(ranks[6:], 2) * blk + jnp.tile(jnp.array([0, blk // 2], I32), 2)
        u_starts = jnp.concatenate([ranks[:6] * blk, split])
        u_all = place(
            [u_f, u_sib, u_x, u_xs, u_y, u_ys, u_d0, u_d1, u_ds0, u_ds1],
            u_starts, n_all)
        tok, coef, loss_row = pl.pallas_call(
            functools.partial(norm_kernel, n_masks, inv_n, shard_rows),
            in_specs=[pl.BlockSpec(memory_space=pltpu.SMEM)] + [pl.BlockSpec(memory_space=pltpu.VMEM)] * 3,
            out_shape=[jax.ShapeDtypeStruct((2, n_own), F32)] * 2 + [jax.ShapeDtypeStruct((1, width), F32)],
        )(plane[None], stats, other, lab_row)
        toks = [tok] + [swap(tok, m) for m in range(1, n_groups)]
        du_part = pl.pallas_call(
            du_kernel, out_shape=tok_f32, compiler_params=vmem_mib(32),
            cost_estimate=cost(SHORT, 10 * n_own * width),
        )(du_sum, label_rows, coef)
        du_other = swap(du_part, 1, "vp")
        norm_all, lab_all = place_toks(toks, ranks)

        nx, nl = SHARE_CHUNKS * SHARE_TILE // 16, LOCAL_TILES * LOCAL_TILE // 16
        assert 16 * (8 * nx + 2 * nl) == shard_rows
        st = SHARE_TILE // 16
        x_at = lambda p, c, k: ((2 * p + c) * nx + k * st)[None]
        y_at = lambda p, c, k: (4 * nx + (2 * p + c) * nx + k * st)[None]
        pad128 = lambda x: jnp.pad(x, ((0, 0), (0, -x.shape[1] % 128)))[:, None, :]
        bias_share = pad128(b_vocab[:16 * 8 * nx].reshape(-1, SHARE_TILE))
        bias_local = pad128(b_vocab[16 * 8 * nx:].reshape(-1, LOCAL_TILE))
        lt = LOCAL_TILE // 16
        out = None

        def rows_call(out, starts, blocks, bias, tile, n_steps, n_send, take):
            return emb_rows(out, starts, blocks, emb_table, bias, u_all, norm_all, lab_all, inv_n, tile, n_steps, n_send,
                            [a for a, _ in take], [s[:1] for _, s in take])

        per = LOCAL_TILES // LOCAL_CALLS
        l_at = lambda c, k: jnp.stack([8 * nx + c * nl + (k * per + i) * lt for i in range(per)])

        def shared_rows(out, k, take):
            starts = jnp.concatenate([x_at(par, core, k), y_at(par, core, k)])
            return rows_call(out, starts, starts // st, bias_share, SHARE_TILE, 2, 2, take)

        def local_rows(out, k, take):
            starts = l_at(core, k)
            out, db, rows = rows_call(out, starts, (starts - 8 * nx) // lt, bias_local, LOCAL_TILE, per, 1, take)
            return out, (swap(rows, 1), l_at(1 - core, k)), db[:, 0, :LOCAL_TILE]

        def near(k, sx, sy):
            return [(swap(sx, 1), x_at(par, 1 - core, k)), (swap(sy, 1), y_at(par, 1 - core, k))]

        def far(k, rx, ry):
            return [(rx, x_at(1 - par, core, k)), (ry, y_at(1 - par, core, k)),
                    (swap(rx, 1), x_at(1 - par, 1 - core, k)),
                    (swap(ry, 1), y_at(1 - par, 1 - core, k))]

        after = lax.optimization_barrier
        out, db0, sx0, sy0 = shared_rows(out, 0, [])
        rx0, ry0 = swap(sx0, 2), swap(sy0, 4)
        near0 = near(0, sx0, sy0)
        out, db1, sx1, sy1 = shared_rows(out, 1, [])
        rx1, ry1 = swap(sx1, 2), swap(sy1, 4)
        near1 = near(1, sx1, sy1)

        du_other, out = after((du_other, out))
        hw = width // 2
        padded = -(-(hw + 4) // 64) * 64
        part = jax.ShapeDtypeStruct((padded // n_groups, width), F32)
        vmem = pl.BlockSpec(memory_space=pltpu.VMEM)
        *parts, d_masked = pl.pallas_call(
            functools.partial(head_kernel, n_groups),
            in_specs=[pl.BlockSpec(memory_space=pltpu.SMEM)] + [vmem] * 7,
            out_shape=[part] * n_groups + [tok_bf16],
            scratch_shapes=[pltpu.VMEM((padded, width), F32)],
            compiler_params=vmem_mib(40),
            cost_estimate=pl.CostEstimate(flops=3 * n_own * width * width, bytes_accessed=20 * n_own * width, transcendentals=2 * n_own * width),
        )(jnp.concatenate([ranks, plane[None]]), pre_act, du_part, du_other, masked_h, w_trans, vectors, loss_row)
        parts, out, d_masked = after((parts, out, d_masked))
        got = [swap(parts[m], m) for m in range(1, n_groups)]

        out, db2, sx2, sy2 = shared_rows(out, 2, [])
        near2 = near(2, sx2, sy2)
        out, rx0, ry0, sx2, sy2 = after((out, rx0, ry0, sx2, sy2))
        rx2, ry2 = swap(sx2, 2), swap(sy2, 4)
        far0 = far(0, rx0, ry0)
        out, db3, sx3, sy3 = shared_rows(out, 3, near0 + near1)
        near3 = near(3, sx3, sy3)
        out, rx1, ry1, sx3, sy3, got = after((out, rx1, ry1, sx3, sy3, got))
        rx3, ry3 = swap(sx3, 2), swap(sy3, 4)
        far1 = far(1, rx1, ry1)
        parts = parts[:1] + got
        level = lambda v: [v[i] + v[i + 1] for i in range(0, len(v), 2)]
        acc = level(level(level(parts)))[0]
        db_mine = jnp.stack([jnp.concatenate([d[i, 0, :SHARE_TILE] for d in (db0, db1, db2, db3)]) for i in range(2)])
        acc, db_mine, out = after((acc, db_mine, out))
        sums = [acc] + [swap(acc, m) for m in range(1, n_groups)]
        db_rel = [db_mine] + [swap(db_mine, m) for m in (1, 2, 3)]
        out, got0, dl0 = local_rows(out, 0, near2 + far0)
        d_hidden = jnp.einsum("clt,cle->cte", pos_onehot, d_masked.reshape(n_rows, SLOTS, width), preferred_element_type=F32).astype(BF16)
        sums, out, d_hidden = after((sums, out, d_hidden))
        w_half, small = join_pieces(sums, ranks, hw)
        w_half, out = after((w_half, out))
        w_other = swap(w_half, 1, "vp")
        out, rx2, ry2, db_rel = after((out, rx2, ry2, db_rel))
        far2 = far(2, rx2, ry2)
        db_sh = jnp.stack(db_rel, 1).reshape(2, 2, 2, 16 * nx)
        db_sh = jnp.where(par == 1, jnp.flip(db_sh, 1), db_sh)
        db_sh = jnp.where(core == 1, jnp.flip(db_sh, 2), db_sh).reshape(2 * 4 * 16 * nx)
        out, got1, dl1 = local_rows(out, 1, near3 + far1 + far2[:2] + [got0])
        d_w_trans = gather_pieces([w_half, w_other], jnp.stack([plane, 1 - plane]).astype(I32)).reshape(width, width)
        out, rx3, ry3, d_w_trans = after((out, rx3, ry3, d_w_trans))
        far3 = far(3, rx3, ry3)
        dl_mine = jnp.concatenate([dl0, dl1]).reshape(16 * nl)
        dl_other = swap(dl_mine, 1)
        put = lambda out, items: copy_rows(out, [a for a, _ in items], [s[:1] for _, s in items])
        out = put(out, far2[2:] + far3[:2])
        d_emb_table = put(out, [got1] + far3[2:])
        mlm_loss = small[3, 0]
        d_b_vocab = jnp.concatenate([db_sh, jnp.where(core == 0, dl_mine, dl_other), jnp.where(core == 0, dl_other, dl_mine)])
        return mlm_loss, d_hidden, d_w_trans, small[0], small[1], small[2], d_emb_table, d_b_vocab

    in_specs = (P("dp"), P("dp"), P("dp"), P(), P(), P(), P(), P("vp"), P("vp"))
    out_specs = (P(), P("dp"), P(), P(), P(), P(), P("vp"), P("vp"))

    return jax.shard_map(local_step, mesh=mesh, in_specs=in_specs, out_specs=out_specs, check_vma=False)
```
